32 devices in a mesh: outer: 4 (over z), inner: 2 (over x), head: 4 (over y, core).
Axes of the slice: x: 2, y: 2, z: 4, core: 2. Of those that a mesh axis runs over, the one named last changes fastest.
Arguments:
- stored_query_rows: bfloat16 [2048, 32, 128], P(('outer', 'inner'), 'head'), may hold values from -12 to 12
- stored_key_rows: bfloat16 [2048, 8, 128], P(('outer', 'inner'), 'head'), may hold values from -12 to 12
- stored_value_rows: bfloat16 [2048, 8, 128], P(('outer', 'inner'), 'head'), may hold values from -6 to 6
- span_order: int32 [16], replicated, may hold values from 0 to 15, each once
Outputs:
- attended: bfloat16 [2048, 32, 128], P(('outer', 'inner'), 'head')
The draws below stay inside these ranges and needn't reach their ends.
Inputs may be any that keep to these rules, and one draw needn't show every extreme that they name: `span_order`: a permutation of the sequence's 16 blocks of 128 tokens.
All inputs are finite; a program needn't handle non-finite values.
Results may differ from the reference program's by a relative error of at most 0.0075.
Values may be sent and summed in bfloat16 or wider, within the bound.
A program may use at most 128 MiB of HBM per device.

```python
import math
import jax
import jax.numpy as jnp
from jax import lax

QUERY_HEADS = 32
KEY_VALUE_HEADS = 8
HEAD_DIMENSION = 128
BLOCK_TOKENS = 128
STORED_BLOCKS = 16
SEQUENCE_TOKENS = 2048


def draw_stored_query_rows(key, part):
    value_matrix = jnp.clip(jax.random.normal(jax.random.fold_in(key, 11), (SEQUENCE_TOKENS, QUERY_HEADS, HEAD_DIMENSION), jnp.float32), -6.0, 6.0)
    return value_matrix.astype(jnp.bfloat16)


def draw_stored_key_rows(key, part):
    value_matrix = jnp.clip(jax.random.normal(jax.random.fold_in(key, 12), (SEQUENCE_TOKENS, KEY_VALUE_HEADS, HEAD_DIMENSION), jnp.float32), -6.0, 6.0)
    return value_matrix.astype(jnp.bfloat16)


def block_levels(key, dims, shards, low, largest):
    level = 1.0
    for position, shards_of in shards:
        draws = jax.random.uniform(jax.random.fold_in(jax.random.fold_in(key, 6), position), (shards_of,), jnp.float32, low / len(shards), largest / len(shards))
        level = level * jnp.repeat(jnp.exp(draws), dims[position] // shards_of).reshape((-1,) + (1,) * (len(dims) - 1 - position))
    return level


def bell_draw(stream_key, dims, width, reach, pieces=(), held_as=jnp.bfloat16):
    entries = jax.random.normal(stream_key, dims, jnp.float32) * width
    if len(pieces) > 0:
        entries = block_levels(stream_key, dims, pieces, -0.22, 0.18) * entries
    return jnp.clip(entries, min=-reach, max=reach).astype(held_as)


def setup_inputs(seed: int = 0) -> dict:
    key_of = jax.random.split(jax.random.key(seed), 5)
    stored_query_rows = draw_stored_query_rows(jax.random.fold_in(key_of[4], 71), 0)
    stored_key_rows = draw_stored_key_rows(jax.random.fold_in(key_of[4], 71), 0)
    stored_value_rows = bell_draw(key_of[2], (SEQUENCE_TOKENS, KEY_VALUE_HEADS, HEAD_DIMENSION), 1.0, 6.0, ((0, 8), (1, 4)))
    span_order = jax.random.permutation(key_of[3], STORED_BLOCKS).astype(jnp.int32)
    return {"stored_query_rows": stored_query_rows, "stored_key_rows": stored_key_rows, "stored_value_rows": stored_value_rows, "span_order": span_order}


def attend_block(carry, query_tile, key_tile, value_tile, allowed, score_scale):
    run_max, run_sum, run_acc = carry
    scores = jnp.einsum('ghqa,kga->ghqk', query_tile.astype(jnp.float32), key_tile.astype(jnp.float32)) * score_scale
    scores = jnp.where(allowed[None, None], scores, -1e+30)
    new_max = jnp.maximum(run_max, lax.optimization_barrier(jnp.max(scores, axis=-1)))
    weights = jnp.where(allowed[None, None], jnp.exp(scores - new_max[..., None]), 0.0)
    rescale = jnp.exp(run_max - new_max)
    new_sum = run_sum * rescale + lax.optimization_barrier(jnp.sum(weights, axis=-1))
    rounded = lax.optimization_barrier(weights.astype(jnp.bfloat16)).astype(jnp.float32)
    added = jnp.einsum('ghqk,kga->ghqa', rounded, value_tile.astype(jnp.float32))
    return (new_max, new_sum, run_acc * rescale[..., None] + added)

def reference(stored_query_rows, stored_key_rows, stored_value_rows, span_order):
    heads_per_group = QUERY_HEADS // KEY_VALUE_HEADS
    inverse_permutation = jnp.zeros((STORED_BLOCKS,), jnp.int32).at[span_order].set(jnp.arange(STORED_BLOCKS, dtype=jnp.int32))
    query_in_order = stored_query_rows.reshape(STORED_BLOCKS, BLOCK_TOKENS, KEY_VALUE_HEADS, heads_per_group, HEAD_DIMENSION)[inverse_permutation].transpose(0, 2, 3, 1, 4)
    key_in_order = stored_key_rows.reshape(STORED_BLOCKS, BLOCK_TOKENS, KEY_VALUE_HEADS, HEAD_DIMENSION)[inverse_permutation]
    value_in_order = stored_value_rows.reshape(STORED_BLOCKS, BLOCK_TOKENS, KEY_VALUE_HEADS, HEAD_DIMENSION)[inverse_permutation]
    score_scale = 1.0 / math.sqrt(HEAD_DIMENSION)
    offsets = jnp.arange(BLOCK_TOKENS, dtype=jnp.int32)

    def one_span(index):
        query_tile = query_in_order[index]

        def visit(block, carry):
            allowed = (block * BLOCK_TOKENS + offsets)[None, :] <= (index * BLOCK_TOKENS + offsets)[:, None]
            return attend_block(carry, query_tile, key_in_order[block], value_in_order[block], allowed, score_scale)
        initial_state = (jnp.full((KEY_VALUE_HEADS, heads_per_group, BLOCK_TOKENS), -1e+30, jnp.float32), jnp.zeros((KEY_VALUE_HEADS, heads_per_group, BLOCK_TOKENS), jnp.float32), jnp.zeros((KEY_VALUE_HEADS, heads_per_group, BLOCK_TOKENS, HEAD_DIMENSION), jnp.float32))
        run_max, run_sum, run_acc = lax.fori_loop(0, index + 1, visit, initial_state)
        return run_acc / run_sum[..., None]
    result = lax.map(one_span, jnp.arange(STORED_BLOCKS, dtype=jnp.int32))
    result = result[span_order]
    return result.transpose(0, 3, 1, 2, 4).reshape(SEQUENCE_TOKENS, QUERY_HEADS, HEAD_DIMENSION).astype(jnp.bfloat16)
```

```python
import functools
import math

import jax
import jax.numpy as jnp
from jax import lax
from jax.experimental import pallas as pl
from jax.experimental.pallas import tpu as pltpu
from jax.sharding import PartitionSpec as P

MESH = pl.DeviceIdType.MESH
MASKED = -1e30
TILE = 512
CHUNKS = 4


def kernel(
    n_outer,
    n_inner,
    heads,
    span_hbm,
    q_ref,
    kv_ref,
    o_ref,
    span_ref,
    span_sem,
    wide_ref,
    held,
    top_ref,
    sum_ref,
    acc_ref,
    send_up,
    send_down,
    send_across,
    send_far,
    recv_sem,
):
    rows, width = q_ref.shape
    kv_rows = kv_ref.shape[0]
    pair = kv_ref.shape[1] // 2
    span = kv_rows // 2
    chunk = kv_rows // CHUNKS
    tiles = rows // TILE
    factor = math.log2(math.e) / math.sqrt(width)
    outer = lax.axis_index("outer")
    inner = lax.axis_index("inner")
    far_halves = n_inner == 2 and n_outer > 2
    last = n_outer - 1

    spans = pltpu.make_async_copy(span_hbm, span_ref, span_sem)
    spans.start()

    barrier = pltpu.get_barrier_semaphore()

    @pl.when(outer > 0)
    def _():
        pl.semaphore_signal(barrier, inc=1, device_id={"outer": outer - 1}, device_id_type=MESH)

    @pl.when(outer < n_outer - 1)
    def _():
        pl.semaphore_signal(barrier, inc=1, device_id={"outer": outer + 1}, device_id_type=MESH)

    for step in range(1, n_inner):
        peer = lax.rem(inner + step, n_inner)
        pl.semaphore_signal(barrier, inc=1, device_id={"inner": peer}, device_id_type=MESH)

    ends = jnp.minimum(outer, 1) + jnp.minimum(n_outer - 1 - outer, 1)
    pl.semaphore_wait(barrier, n_inner - 1 + ends)

    def copy_of(source, src_outer, src_inner, part, send_sem, target):
        return pltpu.make_async_remote_copy(
            src_ref=source.at[pl.ds(part * chunk, chunk)],
            dst_ref=held.at[src_outer, src_inner, pl.ds(part * chunk, chunk)],
            send_sem=send_sem,
            recv_sem=recv_sem.at[src_outer, src_inner, part],
            device_id=target,
            device_id_type=MESH,
        )

    def up(source, src_outer, part):
        return copy_of(
            source, src_outer, inner, part, send_up.at[src_outer, part], {"outer": outer + 1}
        )

    def down(source, src_outer, part):
        return copy_of(
            source, src_outer, inner, part, send_down.at[src_outer, part], {"outer": outer - 1}
        )

    def across(source, src_outer, part, step):
        peer = lax.rem(inner + step, n_inner)
        return copy_of(
            source,
            src_outer,
            inner,
            part,
            send_across.at[src_outer, part, step - 1],
            {"inner": peer},
        )

    def is_far(src_outer):
        return jnp.logical_or(src_outer == 0, src_outer == last)

    def crosses(src_outer, part):
        if not far_halves or part < CHUNKS // 2:
            return jnp.bool_(True)
        return jnp.logical_or(src_outer == outer, jnp.logical_not(is_far(src_outer)))

    def pass_on(source, src_outer, part, act):
        @pl.when(jnp.logical_and(src_outer <= outer, outer < last))
        def _():
            act(up(source, src_outer, part))

        @pl.when(jnp.logical_and(src_outer >= outer, outer > 0))
        def _():
            act(down(source, src_outer, part))

        @pl.when(crosses(src_outer, part))
        def _():
            for step in range(1, n_inner):
                act(across(source, src_outer, part, step))

    def far_on(src_outer, part, act):
        other = n_inner - 1 - inner
        source = held.at[src_outer, other]

        @pl.when(jnp.logical_and(src_outer == 0, outer < last))
        def _():
            act(
                copy_of(
                    source, 0, other, part, send_far.at[0, part], {"outer": outer + 1}
                )
            )

        @pl.when(jnp.logical_and(src_outer == last, outer > 0))
        def _():
            act(
                copy_of(
                    source, last, other, part, send_far.at[1, part], {"outer": outer - 1}
                )
            )

    def arrived(src_outer, src_inner, part):
        place = held.at[src_outer, src_inner, pl.ds(part * chunk, chunk)]
        pltpu.make_async_remote_copy(
            src_ref=place,
            dst_ref=place,
            send_sem=recv_sem.at[src_outer, src_inner, part],
            recv_sem=recv_sem.at[src_outer, src_inner, part],
            device_id={"inner": lax.rem(inner + 1, n_inner)},
            device_id_type=MESH,
        ).wait_recv()

    for part in range(CHUNKS):
        pass_on(kv_ref, outer, part, lambda copy: copy.start())

    spans.wait()

    row_head = lax.rem(lax.broadcasted_iota(jnp.int32, (TILE, width), 0), heads)
    first_head = row_head < heads // 2
    keep_first = jnp.where(first_head, 1.0, 0.0).astype(q_ref.dtype)
    keep_second = jnp.where(first_head, 0.0, 1.0).astype(q_ref.dtype)
    here = (outer * n_inner + inner) * 2
    lane = lax.broadcasted_iota(jnp.int32, (TILE, kv_rows), 1)

    def attend(block, value):
        pv = jnp.dot(block.astype(jnp.bfloat16), value, preferred_element_type=jnp.float32)
        return jnp.where(first_head, pv[:, :width], pv[:, width:])

    def scores_of(wide, key):
        return lax.dot_general(
            wide, key, (((1,), (1,)), ((), ())), preferred_element_type=jnp.float32
        )

    def at(index):
        return pl.ds(index * TILE, TILE)

    def own_scores(index):
        query = q_ref[at(index), :]
        wide = jnp.concatenate([query * keep_first, query * keep_second], axis=1)
        wide_ref[at(index), :] = wide
        return scores_of(wide, kv_ref[:, :pair])

    def visit_own():
        row = lax.broadcasted_iota(jnp.int32, (TILE, kv_rows), 0)
        anchor = jnp.where(lane < span, span_ref[here], span_ref[here + 1])
        ahead = anchor * span + lax.rem(lane, span) - row // heads
        scores = own_scores(0)
        for index in range(tiles):
            following = own_scores(index + 1) if index + 1 < tiles else None
            q_block = index // (tiles // 2)
            q_offset = (index - q_block * (tiles // 2)) * TILE // heads
            allowed = ahead <= span_ref[here + q_block] * span + q_offset
            scores = jnp.where(allowed, scores, MASKED)
            top = jnp.max(scores, axis=1, keepdims=True)
            weights = jnp.exp2((scores - top) * factor)
            top_ref[at(index), :] = jnp.broadcast_to(top, (TILE, width))
            sum_ref[at(index), :] = weights[:, :width] + weights[:, width:]
            acc_ref[at(index), :] = attend(weights, kv_ref[:, pair:])
            scores = following

    visit_own()

    def visit(src_outer, src_inner):
        base = (src_outer * n_inner + src_inner) * 2
        anchors = [span_ref[base], span_ref[base + 1]]
        place = held.at[src_outer, src_inner]

        def settle_sum(index, rescale, added):
            acc_ref[at(index), :] = acc_ref[at(index), :] * rescale + added

        scores = scores_of(wide_ref[at(0), :], place[:, :pair])
        waiting = None
        for index in range(tiles):
            following = None
            if index + 1 < tiles:
                following = scores_of(wide_ref[at(index + 1), :], place[:, :pair])
            q_anchor = span_ref[here + index // (tiles // 2)]
            bias = [jnp.where(anchor < q_anchor, 0.0, MASKED) for anchor in anchors]
            left = scores[:, :width] + bias[0]
            right = scores[:, width:] + bias[1]
            old = top_ref[at(index), :]
            top = jnp.maximum(old, jnp.max(jnp.maximum(left, right), axis=1, keepdims=True))
            rescale = jnp.exp2((old - top) * factor)
            left = jnp.exp2((left - top) * factor)
            right = jnp.exp2((right - top) * factor)
            top_ref[at(index), :] = top
            sum_ref[at(index), :] = sum_ref[at(index), :] * rescale + (left + right)
            weights = jnp.concatenate([left, right], axis=1)
            added = attend(weights, place[:, pair:])
            if waiting is not None:
                settle_sum(*waiting)
            waiting = (index, rescale, added)
            scores = following
        settle_sum(*waiting)

    first_half, second_half = range(CHUNKS // 2), range(CHUNKS // 2, CHUNKS)

    def take(step, parts):
        for part in parts:
            for side in (1, -1):
                src_outer = outer + side * step

                @pl.when(jnp.logical_and(src_outer >= 0, src_outer < n_outer))
                def _():
                    arrived(src_outer, inner, part)
                    pass_on(
                        held.at[src_outer, inner], src_outer, part, lambda copy: copy.start()
                    )

                if far_halves and part >= CHUNKS // 2:

                    @pl.when(src_outer == (n_outer if side == 1 else -1))
                    def _():
                        end = last if side == 1 else 0
                        arrived(end, n_inner - 1 - inner, part)
                        far_on(end, part, lambda copy: copy.start())

    def visit_sides(distance, other):
        def one(side, carry):
            src_outer = outer + (1 - 2 * side) * distance

            @pl.when(
                jnp.logical_and(
                    jnp.logical_and(src_outer >= 0, src_outer < n_outer),
                    jnp.logical_and(distance >= 0, jnp.logical_or(distance > 0, side == 0)),
                )
            )
            def _():
                if not other:
                    visit(src_outer, inner)
                else:

                    def of_inner(step, carry):
                        src_inner = lax.rem(inner + step, n_inner)
                        for part in range(CHUNKS):
                            if far_halves and part >= CHUNKS // 2:

                                @pl.when(jnp.logical_not(is_far(src_outer)))
                                def _():
                                    arrived(src_outer, src_inner, part)
                            else:
                                arrived(src_outer, src_inner, part)
                        visit(src_outer, src_inner)
                        return carry

                    lax.fori_loop(1, n_inner, of_inner, 0)

            return carry

        lax.fori_loop(0, 2, one, 0)

    def line_step(step, carry):
        @pl.when(step > 1)
        def _():
            visit_sides(step - 1, False)

        take(step, first_half)
        visit_sides(step - 2, True)
        take(step, second_half)
        return carry

    lax.fori_loop(1, n_outer + 1, line_step, 0)
    visit_sides(n_outer - 1, True)

    for index in range(tiles):
        total = jnp.sum(sum_ref[at(index), :], axis=1, keepdims=True)
        o_ref[at(index), :] = (acc_ref[at(index), :] / total).astype(o_ref.dtype)

    def settle(src_outer, carry):
        for part in range(CHUNKS):
            pass_on(kv_ref, src_outer, part, lambda copy: copy.wait_send())
        return carry

    lax.fori_loop(0, n_outer, settle, 0)
    if far_halves:
        for part in second_half:
            for end in (0, last):
                far_on(end, part, lambda copy: copy.wait_send())


def solution(mesh):
    n_outer, n_inner = mesh.shape["outer"], mesh.shape["inner"]

    def body(query, key, value, span_order):
        kv_rows, groups, width = key.shape
        heads = query.shape[1]
        rows = query.shape[0] * heads
        kv = jnp.concatenate(
            [key.reshape(kv_rows, groups * width), value.reshape(kv_rows, groups * width)], axis=1
        )
        vmem = pl.BlockSpec(memory_space=pltpu.VMEM)
        out = pl.pallas_call(
            functools.partial(kernel, n_outer, n_inner, heads),
            out_shape=jax.ShapeDtypeStruct((rows, width), jnp.bfloat16),
            in_specs=[pl.BlockSpec(memory_space=pltpu.HBM), vmem, vmem],
            out_specs=vmem,
            scratch_shapes=[
                pltpu.SMEM(span_order.shape, jnp.int32),
                pltpu.SemaphoreType.DMA,
                pltpu.VMEM((rows, groups * width), jnp.bfloat16),
                pltpu.VMEM((n_outer, n_inner) + kv.shape, jnp.bfloat16),
                pltpu.VMEM((rows, width), jnp.float32),
                pltpu.VMEM((rows, width), jnp.float32),
                pltpu.VMEM((rows, width), jnp.float32),
                pltpu.SemaphoreType.DMA((n_outer, CHUNKS)),
                pltpu.SemaphoreType.DMA((n_outer, CHUNKS)),
                pltpu.SemaphoreType.DMA((n_outer, CHUNKS, max(n_inner - 1, 1))),
                pltpu.SemaphoreType.DMA((2, CHUNKS)),
                pltpu.SemaphoreType.DMA((n_outer, n_inner, CHUNKS)),
            ],
            compiler_params=pltpu.CompilerParams(
                collective_id=0, has_side_effects=True, vmem_limit_bytes=48 * 1024 * 1024
            ),
        )(span_order, query.reshape(rows, width), kv)
        return out.reshape(query.shape)

    placed = P(("outer", "inner"), "head", None)
    return jax.shard_map(
        body,
        mesh=mesh,
        in_specs=(placed, placed, placed, P()),
        out_specs=placed,
        check_vma=False,
    )
```

```python
import functools
import math

import jax
import jax.numpy as jnp
from jax import lax
from jax.experimental import pallas as pl
from jax.experimental.pallas import tpu as pltpu
from jax.sharding import PartitionSpec as P

MESH = pl.DeviceIdType.MESH
MASKED = -1e30
VMEM_LIMIT = 48 * 1024 * 1024
CHUNKS = 4


def kernel(
    n_outer,
    n_inner,
    heads,
    span_hbm,
    q_hbm,
    key_hbm,
    value_hbm,
    o_ref,
    span_ref,
    key_ref,
    value_ref,
    q_tiled,
    kv_ref,
    held,
    top_ref,
    sum_ref,
    acc_ref,
    load_sem,
    send_up,
    send_down,
    send_across,
    send_far,
    recv_sem,
):
    tokens, groups, group_heads, width = q_hbm.shape
    q_ref = q_tiled.reshape(groups * tokens * group_heads, width)
    out_ref = o_ref.reshape(groups * tokens * group_heads, width)
    rows = tokens * group_heads
    span = tokens // 2
    chunk = kv_ref.shape[0] // CHUNKS
    tile = rows // 2
    factor = math.log2(math.e) / math.sqrt(width)
    outer = lax.axis_index("outer")
    inner = lax.axis_index("inner")
    far_halves = n_inner == 2 and n_outer > 2
    last = n_outer - 1

    loads = [
        pltpu.make_async_copy(key_hbm, key_ref, load_sem.at[0]),
        pltpu.make_async_copy(value_hbm, value_ref, load_sem.at[1]),
        pltpu.make_async_copy(span_hbm, span_ref, load_sem.at[2]),
    ]
    for group in range(groups):
        loads.append(
            pltpu.make_async_copy(q_hbm.at[:, group], q_tiled.at[group], load_sem.at[3 + group])
        )
    for load in loads:
        load.start()

    barrier = pltpu.get_barrier_semaphore()

    @pl.when(outer > 0)
    def _():
        pl.semaphore_signal(barrier, inc=1, device_id={"outer": outer - 1}, device_id_type=MESH)

    @pl.when(outer < n_outer - 1)
    def _():
        pl.semaphore_signal(barrier, inc=1, device_id={"outer": outer + 1}, device_id_type=MESH)

    for step in range(1, n_inner):
        peer = lax.rem(inner + step, n_inner)
        pl.semaphore_signal(barrier, inc=1, device_id={"inner": peer}, device_id_type=MESH)

    loads[0].wait()
    loads[1].wait()
    for group in range(groups):
        every = pl.ds(group, tokens, stride=groups)
        here_rows = pl.ds(group * tokens, tokens)
        kv_ref[here_rows, :width] = key_ref[every, :]
        kv_ref[here_rows, width:] = value_ref[every, :]

    ends = jnp.minimum(outer, 1) + jnp.minimum(n_outer - 1 - outer, 1)
    pl.semaphore_wait(barrier, n_inner - 1 + ends)

    def copy_of(source, src_outer, src_inner, part, send_sem, target):
        return pltpu.make_async_remote_copy(
            src_ref=source.at[pl.ds(part * chunk, chunk)],
            dst_ref=held.at[src_outer, src_inner, pl.ds(part * chunk, chunk)],
            send_sem=send_sem,
            recv_sem=recv_sem.at[src_outer, src_inner, part],
            device_id=target,
            device_id_type=MESH,
        )

    def up(source, src_outer, part):
        return copy_of(
            source, src_outer, inner, part, send_up.at[src_outer, part], {"outer": outer + 1}
        )

    def down(source, src_outer, part):
        return copy_of(
            source, src_outer, inner, part, send_down.at[src_outer, part], {"outer": outer - 1}
        )

    def across(source, src_outer, part, step):
        peer = lax.rem(inner + step, n_inner)
        return copy_of(
            source,
            src_outer,
            inner,
            part,
            send_across.at[src_outer, part, step - 1],
            {"inner": peer},
        )

    def is_far(src_outer):
        return jnp.logical_or(src_outer == 0, src_outer == last)

    def crosses(src_outer, part):
        if not far_halves or part < CHUNKS // 2:
            return jnp.bool_(True)
        return jnp.logical_or(src_outer == outer, jnp.logical_not(is_far(src_outer)))

    def pass_on(source, src_outer, part, act):
        @pl.when(jnp.logical_and(src_outer <= outer, outer < last))
        def _():
            act(up(source, src_outer, part))

        @pl.when(jnp.logical_and(src_outer >= outer, outer > 0))
        def _():
            act(down(source, src_outer, part))

        @pl.when(crosses(src_outer, part))
        def _():
            for step in range(1, n_inner):
                act(across(source, src_outer, part, step))

    def far_on(src_outer, part, act):
        other = n_inner - 1 - inner
        source = held.at[src_outer, other]

        @pl.when(jnp.logical_and(src_outer == 0, outer < last))
        def _():
            act(
                copy_of(
                    source, 0, other, part, send_far.at[0, part], {"outer": outer + 1}
                )
            )

        @pl.when(jnp.logical_and(src_outer == last, outer > 0))
        def _():
            act(
                copy_of(
                    source, last, other, part, send_far.at[1, part], {"outer": outer - 1}
                )
            )

    def arrived(src_outer, src_inner, part):
        place = held.at[src_outer, src_inner, pl.ds(part * chunk, chunk)]
        pltpu.make_async_remote_copy(
            src_ref=place,
            dst_ref=place,
            send_sem=recv_sem.at[src_outer, src_inner, part],
            recv_sem=recv_sem.at[src_outer, src_inner, part],
            device_id={"inner": lax.rem(inner + 1, n_inner)},
            device_id_type=MESH,
        ).wait_recv()

    for part in range(CHUNKS):
        pass_on(kv_ref, outer, part, lambda copy: copy.start())

    for load in loads[2:]:
        load.wait()

    here = (outer * n_inner + inner) * 2
    lane = lax.broadcasted_iota(jnp.int32, (tile, tokens), 1)
    tiles = [(group, block) for group in range(groups) for block in range(2)]

    def at(index):
        return pl.ds(index * tile, tile)

    def scores_of(index, place):
        group = tiles[index][0]
        return lax.dot_general(
            q_ref[at(index), :],
            place[pl.ds(group * tokens, tokens), :width],
            (((1,), (1,)), ((), ())),
            preferred_element_type=jnp.float32,
        )

    def attend(index, weights, place):
        group = tiles[index][0]
        return jnp.dot(
            weights.astype(jnp.bfloat16),
            place[pl.ds(group * tokens, tokens), width:],
            preferred_element_type=jnp.float32,
        )

    def visit_own():
        row = lax.broadcasted_iota(jnp.int32, (tile, tokens), 0)
        anchor = jnp.where(lane < span, span_ref[here], span_ref[here + 1])
        ahead = anchor * span + lax.rem(lane, span) - row // group_heads
        scores = scores_of(0, kv_ref)
        for index, (group, block) in enumerate(tiles):
            following = scores_of(index + 1, kv_ref) if index + 1 < len(tiles) else None
            scores = jnp.where(ahead <= span_ref[here + block] * span, scores, MASKED)
            top = jnp.max(scores, axis=1, keepdims=True)
            weights = jnp.exp2((scores - top) * factor)
            top_ref[at(index), :] = jnp.broadcast_to(top, (tile, width))
            sum_ref[at(index), :] = weights[:, :width] + weights[:, width:]
            acc_ref[at(index), :] = attend(index, weights, kv_ref)
            scores = following

    visit_own()

    def visit(src_outer, src_inner):
        base = (src_outer * n_inner + src_inner) * 2
        anchors = [span_ref[base], span_ref[base + 1]]
        place = held.at[src_outer, src_inner]

        def settle_sum(index, rescale, added):
            acc_ref[at(index), :] = acc_ref[at(index), :] * rescale + added

        scores = scores_of(0, place)
        waiting = None
        for index, (group, block) in enumerate(tiles):
            following = scores_of(index + 1, place) if index + 1 < len(tiles) else None
            q_anchor = span_ref[here + block]
            bias = [jnp.where(anchor < q_anchor, 0.0, MASKED) for anchor in anchors]
            left = scores[:, :span] + bias[0]
            right = scores[:, span:] + bias[1]
            old = top_ref[at(index), :]
            top = jnp.maximum(old, jnp.max(jnp.maximum(left, right), axis=1, keepdims=True))
            rescale = jnp.exp2((old - top) * factor)
            left = jnp.exp2((left - top) * factor)
            right = jnp.exp2((right - top) * factor)
            top_ref[at(index), :] = top
            sum_ref[at(index), :] = sum_ref[at(index), :] * rescale + (left + right)
            added = attend(index, jnp.concatenate([left, right], axis=1), place)
            if waiting is not None:
                settle_sum(*waiting)
            waiting = (index, rescale, added)
            scores = following
        settle_sum(*waiting)

    first_half, second_half = range(CHUNKS // 2), range(CHUNKS // 2, CHUNKS)

    def take(step, parts):
        for part in parts:
            for side in (1, -1):
                src_outer = outer + side * step

                @pl.when(jnp.logical_and(src_outer >= 0, src_outer < n_outer))
                def _():
                    arrived(src_outer, inner, part)
                    pass_on(
                        held.at[src_outer, inner], src_outer, part, lambda copy: copy.start()
                    )

                if far_halves and part >= CHUNKS // 2:

                    @pl.when(src_outer == (n_outer if side == 1 else -1))
                    def _():
                        end = last if side == 1 else 0
                        arrived(end, n_inner - 1 - inner, part)
                        far_on(end, part, lambda copy: copy.start())

    def visit_sides(distance, other):
        def one(side, carry):
            src_outer = outer + (1 - 2 * side) * distance

            @pl.when(
                jnp.logical_and(
                    jnp.logical_and(src_outer >= 0, src_outer < n_outer),
                    jnp.logical_and(distance >= 0, jnp.logical_or(distance > 0, side == 0)),
                )
            )
            def _():
                if not other:
                    visit(src_outer, inner)
                else:

                    def of_inner(step, carry):
                        src_inner = lax.rem(inner + step, n_inner)
                        for part in range(CHUNKS):
                            if far_halves and part >= CHUNKS // 2:

                                @pl.when(jnp.logical_not(is_far(src_outer)))
                                def _():
                                    arrived(src_outer, src_inner, part)
                            else:
                                arrived(src_outer, src_inner, part)
                        visit(src_outer, src_inner)
                        return carry

                    lax.fori_loop(1, n_inner, of_inner, 0)

            return carry

        lax.fori_loop(0, 2, one, 0)

    def line_step(step, carry):
        @pl.when(step > 1)
        def _():
            visit_sides(step - 1, False)

        take(step, first_half)
        visit_sides(step - 2, True)
        take(step, second_half)
        return carry

    lax.fori_loop(1, n_outer + 1, line_step, 0)
    visit_sides(n_outer - 1, True)

    for index in range(len(tiles)):
        total = jnp.sum(sum_ref[at(index), :], axis=1, keepdims=True)
        out_ref[at(index), :] = (acc_ref[at(index), :] / total).astype(o_ref.dtype)

    def settle(src_outer, carry):
        for part in range(CHUNKS):
            pass_on(kv_ref, src_outer, part, lambda copy: copy.wait_send())
        return carry

    lax.fori_loop(0, n_outer, settle, 0)
    if far_halves:
        for part in second_half:
            for end in (0, last):
                far_on(end, part, lambda copy: copy.wait_send())


def spread(o_ref, out_hbm, sem):
    copies = [
        pltpu.make_async_copy(o_ref.at[group], out_hbm.at[:, group], sem.at[group])
        for group in range(o_ref.shape[0])
    ]
    for copy in copies:
        copy.start()
    for copy in copies:
        copy.wait()


def solution(mesh):
    n_outer, n_inner = mesh.shape["outer"], mesh.shape["inner"]

    def body(query, key, value, span_order):
        tokens, groups, width = key.shape
        heads = query.shape[1]
        group_heads = heads // groups
        rows = tokens * heads
        by_group = (groups, tokens, group_heads, width)
        kv_shape = (groups * tokens, 2 * width)
        vmem = pl.BlockSpec(memory_space=pltpu.VMEM)
        hbm = pl.BlockSpec(memory_space=pltpu.HBM)
        out = pl.pallas_call(
            functools.partial(kernel, n_outer, n_inner, heads),
            out_shape=jax.ShapeDtypeStruct(by_group, jnp.bfloat16),
            in_specs=[hbm] * 4,
            out_specs=vmem,
            scratch_shapes=[
                pltpu.SMEM(span_order.shape, jnp.int32),
                pltpu.VMEM((groups * tokens, width), jnp.bfloat16),
                pltpu.VMEM((groups * tokens, width), jnp.bfloat16),
                pltpu.VMEM(by_group, jnp.bfloat16),
                pltpu.VMEM(kv_shape, jnp.bfloat16),
                pltpu.VMEM((n_outer, n_inner) + kv_shape, jnp.bfloat16),
                pltpu.VMEM((rows, width), jnp.float32),
                pltpu.VMEM((rows, width), jnp.float32),
                pltpu.VMEM((rows, width), jnp.float32),
                pltpu.SemaphoreType.DMA((3 + groups,)),
                pltpu.SemaphoreType.DMA((n_outer, CHUNKS)),
                pltpu.SemaphoreType.DMA((n_outer, CHUNKS)),
                pltpu.SemaphoreType.DMA((n_outer, CHUNKS, max(n_inner - 1, 1))),
                pltpu.SemaphoreType.DMA((2, CHUNKS)),
                pltpu.SemaphoreType.DMA((n_outer, n_inner, CHUNKS)),
            ],
            compiler_params=pltpu.CompilerParams(
                collective_id=0, has_side_effects=True, vmem_limit_bytes=VMEM_LIMIT
            ),
        )(
            pltpu.with_memory_space_constraint(span_order, pltpu.HBM),
            pltpu.with_memory_space_constraint(query.reshape(tokens, groups, group_heads, width), pltpu.HBM),
            pltpu.with_memory_space_constraint(key.reshape(groups * tokens, width), pltpu.HBM),
            pltpu.with_memory_space_constraint(value.reshape(groups * tokens, width), pltpu.HBM),
        )
        out = pl.pallas_call(
            spread,
            out_shape=jax.ShapeDtypeStruct((tokens, groups, group_heads, width), jnp.bfloat16),
            in_specs=[vmem],
            out_specs=hbm,
            scratch_shapes=[pltpu.SemaphoreType.DMA((groups,))],
            compiler_params=pltpu.CompilerParams(vmem_limit_bytes=1024 * 1024),
        )(out)
        return out.reshape(query.shape)

    placed = P(("outer", "inner"), "head", None)
    return jax.shard_map(
        body,
        mesh=mesh,
        in_specs=(placed, placed, placed, P()),
        out_specs=placed,
        check_vma=False,
    )
```

```python
import functools
import math

import jax
import jax.numpy as jnp
from jax import lax
from jax.experimental import pallas as pl
from jax.experimental.pallas import tpu as pltpu
from jax.sharding import PartitionSpec as P

MESH = pl.DeviceIdType.MESH
MASKED = -1e30
VMEM_LIMIT = 48 * 1024 * 1024
CHUNKS = 4


def kernel(
    n_outer,
    n_inner,
    heads,
    span_hbm,
    q_hbm,
    key_hbm,
    value_hbm,
    o_ref,
    span_ref,
    key_ref,
    value_ref,
    q_tiled,
    q_ref,
    kv_ref,
    held,
    top_ref,
    sum_ref,
    acc_ref,
    load_sem,
    send_sem,
    recv_sem,
):
    tokens, groups, group_heads, width = q_hbm.shape
    q_rows = q_tiled.reshape(groups * tokens * group_heads, width)
    out_ref = o_ref.reshape(groups * tokens * group_heads, width)
    rows = tokens * group_heads
    span = tokens // 2
    chunk = kv_ref.shape[0] // CHUNKS
    tile = rows // 2
    factor = math.log2(math.e) / math.sqrt(width)
    outer = lax.axis_index("outer")
    inner = lax.axis_index("inner")
    far_halves = n_inner == 2 and n_outer > 2
    last = n_outer - 1

    loads = [
        pltpu.make_async_copy(key_hbm, key_ref, load_sem.at[0]),
        pltpu.make_async_copy(value_hbm, value_ref, load_sem.at[1]),
        pltpu.make_async_copy(span_hbm, span_ref, load_sem.at[2]),
    ]
    for group in range(groups):
        loads.append(
            pltpu.make_async_copy(q_hbm.at[:, group], q_tiled.at[group], load_sem.at[3])
        )
    for load in loads:
        load.start()

    barrier = pltpu.get_barrier_semaphore()

    @pl.when(outer > 0)
    def _():
        pl.semaphore_signal(barrier, inc=1, device_id={"outer": outer - 1}, device_id_type=MESH)

    @pl.when(outer < n_outer - 1)
    def _():
        pl.semaphore_signal(barrier, inc=1, device_id={"outer": outer + 1}, device_id_type=MESH)

    for step in range(1, n_inner):
        peer = lax.rem(inner + step, n_inner)
        pl.semaphore_signal(barrier, inc=1, device_id={"inner": peer}, device_id_type=MESH)

    loads[0].wait()
    loads[1].wait()
    for group in range(groups):
        every = pl.ds(group, tokens, stride=groups)
        here_rows = pl.ds(group * tokens, tokens)
        kv_ref[here_rows, :width] = key_ref[every, :]
        kv_ref[here_rows, width:] = value_ref[every, :]

    ends = jnp.minimum(outer, 1) + jnp.minimum(n_outer - 1 - outer, 1)
    pl.semaphore_wait(barrier, n_inner - 1 + ends)

    def copy_of(source, src_outer, src_inner, part, target):
        return pltpu.make_async_remote_copy(
            src_ref=source.at[pl.ds(part * chunk, chunk)],
            dst_ref=held.at[src_outer, src_inner, pl.ds(part * chunk, chunk)],
            send_sem=send_sem,
            recv_sem=recv_sem.at[src_outer, src_inner, part],
            device_id=target,
            device_id_type=MESH,
        )

    def up(source, src_outer, part):
        return copy_of(source, src_outer, inner, part, {"outer": outer + 1})

    def down(source, src_outer, part):
        return copy_of(source, src_outer, inner, part, {"outer": outer - 1})

    def across(source, src_outer, part, step):
        peer = lax.rem(inner + step, n_inner)
        return copy_of(source, src_outer, inner, part, {"inner": peer})

    def is_far(src_outer):
        return jnp.logical_or(src_outer == 0, src_outer == last)

    def crosses(src_outer, part):
        if not far_halves or part < CHUNKS // 2:
            return jnp.bool_(True)
        return jnp.logical_or(src_outer == outer, jnp.logical_not(is_far(src_outer)))

    def pass_on(source, src_outer, part, act):
        going_up = jnp.logical_and(src_outer <= outer, outer < last)
        going_down = jnp.logical_and(src_outer >= outer, outer > 0)
        upper = outer >= n_outer // 2

        @pl.when(jnp.logical_and(going_up, upper))
        def _():
            act(up(source, src_outer, part))

        @pl.when(going_down)
        def _():
            act(down(source, src_outer, part))

        @pl.when(crosses(src_outer, part))
        def _():
            for step in range(1, n_inner):
                act(across(source, src_outer, part, step))

        @pl.when(jnp.logical_and(going_up, jnp.logical_not(upper)))
        def _():
            act(up(source, src_outer, part))

    def far_on(src_outer, part, act):
        other = n_inner - 1 - inner
        source = held.at[src_outer, other]

        @pl.when(jnp.logical_and(src_outer == 0, outer < last))
        def _():
            act(copy_of(source, 0, other, part, {"outer": outer + 1}))

        @pl.when(jnp.logical_and(src_outer == last, outer > 0))
        def _():
            act(copy_of(source, last, other, part, {"outer": outer - 1}))

    def arrived(src_outer, src_inner, part):
        place = held.at[src_outer, src_inner, pl.ds(part * chunk, chunk)]
        pltpu.make_async_remote_copy(
            src_ref=place,
            dst_ref=place,
            send_sem=recv_sem.at[src_outer, src_inner, part],
            recv_sem=recv_sem.at[src_outer, src_inner, part],
            device_id={"inner": lax.rem(inner + 1, n_inner)},
            device_id_type=MESH,
        ).wait_recv()

    for part in range(CHUNKS):
        pass_on(kv_ref, outer, part, lambda copy: copy.start())

    loads[2].wait()
    pltpu.make_async_copy(q_tiled, q_tiled, load_sem.at[3]).wait()

    here = (outer * n_inner + inner) * 2
    lane = lax.broadcasted_iota(jnp.int32, (tile, tokens), 1)
    tiles = [(group, block) for group in range(groups) for block in range(2)]

    def at(group, block):
        return pl.ds((group * 2 + block) * tile, tile)

    column = lax.broadcasted_iota(jnp.int32, (tile, width), 1)
    for group, block in tiles:
        q_ref[at(group, block), :width] = q_rows[at(group, block), :]
        q_ref[at(group, block), width:] = jnp.where(column == block, 1.0, 0.0).astype(q_ref.dtype)

    def biases(base):
        column = lax.broadcasted_iota(jnp.int32, (span, width), 1)
        halves = []
        for half in range(2):
            bias = [
                jnp.where(span_ref[base + half] < span_ref[here + block], 0.0, MASKED)
                for block in range(2)
            ]
            halves.append(jnp.where(column == 0, bias[0], jnp.where(column == 1, bias[1], 0.0)))
        return jnp.concatenate(halves, axis=0).astype(kv_ref.dtype)

    def scores_of(group, block, place, bias=None):
        keys = place[pl.ds(group * tokens, tokens), :width]
        queries = q_ref[at(group, block), :width]
        if bias is not None:
            keys = jnp.concatenate([keys, bias], axis=1)
            queries = q_ref[at(group, block), :]
        return lax.dot_general(
            queries, keys, (((1,), (1,)), ((), ())), preferred_element_type=jnp.float32
        )

    def attend(group, weights, place):
        return jnp.dot(
            weights.astype(jnp.bfloat16),
            place[pl.ds(group * tokens, tokens), width:],
            preferred_element_type=jnp.float32,
        )

    def visit_own():
        row = lax.broadcasted_iota(jnp.int32, (tile, tokens), 0)
        anchor = jnp.where(lane < span, span_ref[here], span_ref[here + 1])
        ahead = anchor * span + lax.rem(lane, span) - row // group_heads
        scores = scores_of(*tiles[0], kv_ref)
        for index, (group, block) in enumerate(tiles):
            following = None
            if index + 1 < len(tiles):
                following = scores_of(*tiles[index + 1], kv_ref)
            some = at(group, block)
            scores = jnp.where(ahead <= span_ref[here + block] * span, scores, MASKED)
            top = jnp.max(scores, axis=1, keepdims=True)
            weights = jnp.exp2((scores - top) * factor)
            top_ref[some, :] = jnp.broadcast_to(top, (tile, width))
            sum_ref[some, :] = weights[:, :width] + weights[:, width:]
            acc_ref[some, :] = attend(group, weights, kv_ref)
            scores = following

    visit_own()

    def visit(src_outer, src_inner, group, final=False):
        bias = biases((src_outer * n_inner + src_inner) * 2)
        place = held.at[src_outer, src_inner]

        def settle_sum(some, rescale, added, sums):
            acc = acc_ref[some, :] * rescale + added
            if final:
                total = jnp.sum(sums, axis=1, keepdims=True)
                out_ref[some, :] = (acc / total).astype(o_ref.dtype)
            else:
                acc_ref[some, :] = acc

        scores = scores_of(group, 0, place, bias)
        waiting = None
        for block in range(2):
            following = scores_of(group, 1, place, bias) if block == 0 else None
            some = at(group, block)
            left, right = scores[:, :span], scores[:, span:]
            old = top_ref[some, :]
            top = jnp.maximum(old, jnp.max(jnp.maximum(left, right), axis=1, keepdims=True))
            rescale = jnp.exp2((old - top) * factor)
            left = jnp.exp2((left - top) * factor)
            right = jnp.exp2((right - top) * factor)
            sums = sum_ref[some, :] * rescale + (left + right)
            if not final:
                top_ref[some, :] = top
                sum_ref[some, :] = sums
            added = attend(group, jnp.concatenate([left, right], axis=1), place)
            if waiting is not None:
                settle_sum(*waiting)
            waiting = (some, rescale, added, sums)
            scores = following
        settle_sum(*waiting)

    end_outer = jnp.where(outer < n_outer // 2, last, 0)
    first_half, second_half = range(CHUNKS // 2), range(CHUNKS // 2, CHUNKS)
    parts_of = [first_half, second_half]

    def take(step, parts):
        for part in parts:
            for side in (1, -1):
                src_outer = outer + side * step

                @pl.when(jnp.logical_and(src_outer >= 0, src_outer < n_outer))
                def _():
                    arrived(src_outer, inner, part)
                    pass_on(
                        held.at[src_outer, inner], src_outer, part, lambda copy: copy.start()
                    )

    def take_far(step):
        for side, end in ((1, last), (-1, 0)):

            @pl.when(outer + side * step == end + side)
            def _():
                for part in second_half:
                    arrived(end, n_inner - 1 - inner, part)
                    far_on(end, part, lambda copy: copy.start())

    def sides(distance, act):
        def one(side, carry):
            src_outer = outer + (1 - 2 * side) * distance

            @pl.when(
                jnp.logical_and(
                    jnp.logical_and(src_outer >= 0, src_outer < n_outer),
                    jnp.logical_and(distance >= 0, jnp.logical_or(distance > 0, side == 0)),
                )
            )
            def _():
                act(src_outer)

            return carry

        lax.fori_loop(0, 2, one, 0)

    def visit_others(src_outer):
        def of_inner(step, carry):
            src_inner = lax.rem(inner + step, n_inner)
            for group in range(groups):
                for part in parts_of[group]:
                    if far_halves and group > 0:

                        @pl.when(jnp.logical_not(is_far(src_outer)))
                        def _():
                            arrived(src_outer, src_inner, part)
                    else:
                        arrived(src_outer, src_inner, part)
                visit(src_outer, src_inner, group)
            return carry

        until = jnp.where(src_outer == end_outer, n_inner - 1, n_inner)
        lax.fori_loop(1, until, of_inner, 0)

    def line_step(step, carry):
        take(step, first_half)
        if far_halves:
            take_far(step)
        sides(step, lambda src_outer: visit(src_outer, inner, 0))
        sides(step - 2 + jnp.where(is_far(outer), 1, 0), visit_others)
        take(step, second_half)
        sides(step, lambda src_outer: visit(src_outer, inner, 1))
        return carry

    lax.fori_loop(1, n_outer, line_step, 0)
    if n_inner > 2:
        sides(jnp.abs(end_outer - outer), visit_others)

    end_inner = lax.rem(inner + n_inner - 1, n_inner)
    for group in range(groups):
        for part in parts_of[group]:
            if far_halves and group > 0:

                @pl.when(is_far(outer))
                def _():
                    arrived(end_outer, end_inner, part)
            else:
                arrived(end_outer, end_inner, part)
        visit(end_outer, end_inner, group, final=True)

    def settle(src_outer, carry):
        for part in range(CHUNKS):
            pass_on(kv_ref, src_outer, part, lambda copy: copy.wait_send())
        return carry

    lax.fori_loop(0, n_outer, settle, 0)
    if far_halves:
        for part in second_half:
            for end in (0, last):
                far_on(end, part, lambda copy: copy.wait_send())


def spread(o_ref, out_hbm, sem):
    copies = [
        pltpu.make_async_copy(o_ref.at[group], out_hbm.at[:, group], sem.at[group])
        for group in range(o_ref.shape[0])
    ]
    for copy in copies:
        copy.start()
    for copy in copies:
        copy.wait()


def solution(mesh):
    n_outer, n_inner = mesh.shape["outer"], mesh.shape["inner"]

    def body(query, key, value, span_order):
        tokens, groups, width = key.shape
        heads = query.shape[1]
        group_heads = heads // groups
        rows = tokens * heads
        by_group = (groups, tokens, group_heads, width)
        kv_shape = (groups * tokens, 2 * width)
        vmem = pl.BlockSpec(memory_space=pltpu.VMEM)
        hbm = pl.BlockSpec(memory_space=pltpu.HBM)
        out = pl.pallas_call(
            functools.partial(kernel, n_outer, n_inner, heads),
            out_shape=jax.ShapeDtypeStruct(by_group, jnp.bfloat16),
            in_specs=[hbm] * 4,
            out_specs=vmem,
            scratch_shapes=[
                pltpu.SMEM(span_order.shape, jnp.int32),
                pltpu.VMEM((groups * tokens, width), jnp.bfloat16),
                pltpu.VMEM((groups * tokens, width), jnp.bfloat16),
                pltpu.VMEM(by_group, jnp.bfloat16),
                pltpu.VMEM((rows, 2 * width), jnp.bfloat16),
                pltpu.VMEM(kv_shape, jnp.bfloat16),
                pltpu.VMEM((n_outer, n_inner) + kv_shape, jnp.bfloat16),
                pltpu.VMEM((rows, width), jnp.float32),
                pltpu.VMEM((rows, width), jnp.float32),
                pltpu.VMEM((rows, width), jnp.float32),
                pltpu.SemaphoreType.DMA((4,)),
                pltpu.SemaphoreType.DMA,
                pltpu.SemaphoreType.DMA((n_outer, n_inner, CHUNKS)),
            ],
            compiler_params=pltpu.CompilerParams(
                collective_id=0, has_side_effects=True, vmem_limit_bytes=VMEM_LIMIT
            ),
        )(
            pltpu.with_memory_space_constraint(span_order, pltpu.HBM),
            pltpu.with_memory_space_constraint(query.reshape(tokens, groups, group_heads, width), pltpu.HBM),
            pltpu.with_memory_space_constraint(key.reshape(groups * tokens, width), pltpu.HBM),
            pltpu.with_memory_space_constraint(value.reshape(groups * tokens, width), pltpu.HBM),
        )
        out = pl.pallas_call(
            spread,
            out_shape=jax.ShapeDtypeStruct((tokens, groups, group_heads, width), jnp.bfloat16),
            in_specs=[vmem],
            out_specs=hbm,
            scratch_shapes=[pltpu.SemaphoreType.DMA((groups,))],
            compiler_params=pltpu.CompilerParams(vmem_limit_bytes=1024 * 1024),
        )(out)
        return out.reshape(query.shape)

    placed = P(("outer", "inner"), "head", None)
    return jax.shard_map(
        body,
        mesh=mesh,
        in_specs=(placed, placed, placed, P()),
        out_specs=placed,
        check_vma=False,
    )
```

```python
import functools
import math

import jax
import jax.numpy as jnp
from jax import lax
from jax.experimental import pallas as pl
from jax.experimental.pallas import tpu as pltpu
from jax.sharding import PartitionSpec as P

MESH = pl.DeviceIdType.MESH
MASKED = -1e30
VMEM_LIMIT = 48 * 1024 * 1024
CHUNKS = 4


def kernel(
    n_outer,
    n_inner,
    heads,
    span_hbm,
    q_hbm,
    key_hbm,
    value_hbm,
    o_ref,
    span_ref,
    key_ref,
    value_ref,
    q_tiled,
    q_ref,
    kv_ref,
    held,
    top_ref,
    sum_ref,
    acc_ref,
    load_sem,
    send_sem,
    recv_sem,
):
    tokens, groups, group_heads, width = q_hbm.shape
    q_rows = q_tiled.reshape(groups * tokens * group_heads, width)
    out_ref = o_ref.reshape(groups * tokens * group_heads, width)
    rows = tokens * group_heads
    span = tokens // 2
    chunk = kv_ref.shape[0] // CHUNKS
    tile = rows // 2
    factor = math.log2(math.e) / math.sqrt(width)
    outer = lax.axis_index("outer")
    inner = lax.axis_index("inner")
    far_halves = n_inner == 2 and n_outer > 2
    last = n_outer - 1

    loads = [
        pltpu.make_async_copy(key_hbm, key_ref, load_sem.at[0]),
        pltpu.make_async_copy(value_hbm, value_ref, load_sem.at[1]),
        pltpu.make_async_copy(span_hbm, span_ref, load_sem.at[2]),
    ]
    for group in range(groups):
        loads.append(
            pltpu.make_async_copy(q_hbm.at[:, group], q_tiled.at[group], load_sem.at[3])
        )
    for load in loads:
        load.start()

    barrier = pltpu.get_barrier_semaphore()

    @pl.when(outer > 0)
    def _():
        pl.semaphore_signal(barrier, inc=1, device_id={"outer": outer - 1}, device_id_type=MESH)

    @pl.when(outer < n_outer - 1)
    def _():
        pl.semaphore_signal(barrier, inc=1, device_id={"outer": outer + 1}, device_id_type=MESH)

    for step in range(1, n_inner):
        peer = lax.rem(inner + step, n_inner)
        pl.semaphore_signal(barrier, inc=1, device_id={"inner": peer}, device_id_type=MESH)

    loads[0].wait()
    loads[1].wait()
    for group in range(groups):
        every = pl.ds(group, tokens, stride=groups)
        here_rows = pl.ds(group * tokens, tokens)
        kv_ref[here_rows, :width] = key_ref[every, :]
        kv_ref[here_rows, width:] = value_ref[every, :]

    ends = jnp.minimum(outer, 1) + jnp.minimum(n_outer - 1 - outer, 1)
    pl.semaphore_wait(barrier, n_inner - 1 + ends)

    def copy_of(source, src_outer, src_inner, part, target):
        return pltpu.make_async_remote_copy(
            src_ref=source.at[pl.ds(part * chunk, chunk)],
            dst_ref=held.at[src_outer, src_inner, pl.ds(part * chunk, chunk)],
            send_sem=send_sem,
            recv_sem=recv_sem.at[src_outer, src_inner, part],
            device_id=target,
            device_id_type=MESH,
        )

    def up(source, src_outer, part):
        return copy_of(source, src_outer, inner, part, {"outer": outer + 1})

    def down(source, src_outer, part):
        return copy_of(source, src_outer, inner, part, {"outer": outer - 1})

    def across(source, src_outer, part, step):
        peer = lax.rem(inner + step, n_inner)
        return copy_of(source, src_outer, inner, part, {"inner": peer})

    def is_far(src_outer):
        return jnp.logical_or(src_outer == 0, src_outer == last)

    def crosses(src_outer, part):
        if not far_halves or part < CHUNKS // 2:
            return jnp.bool_(True)
        return jnp.logical_or(src_outer == outer, jnp.logical_not(is_far(src_outer)))

    def pass_on(source, src_outer, part, act):
        going_up = jnp.logical_and(src_outer <= outer, outer < last)
        going_down = jnp.logical_and(src_outer >= outer, outer > 0)
        upper = outer >= n_outer // 2

        @pl.when(jnp.logical_and(going_up, upper))
        def _():
            act(up(source, src_outer, part))

        @pl.when(going_down)
        def _():
            act(down(source, src_outer, part))

        @pl.when(crosses(src_outer, part))
        def _():
            for step in range(1, n_inner):
                act(across(source, src_outer, part, step))

        @pl.when(jnp.logical_and(going_up, jnp.logical_not(upper)))
        def _():
            act(up(source, src_outer, part))

    def far_on(src_outer, part, act):
        other = n_inner - 1 - inner
        source = held.at[src_outer, other]

        @pl.when(jnp.logical_and(src_outer == 0, outer < last))
        def _():
            act(copy_of(source, 0, other, part, {"outer": outer + 1}))

        @pl.when(jnp.logical_and(src_outer == last, outer > 0))
        def _():
            act(copy_of(source, last, other, part, {"outer": outer - 1}))

    def arrived(src_outer, src_inner, part):
        place = held.at[src_outer, src_inner, pl.ds(part * chunk, chunk)]
        pltpu.make_async_remote_copy(
            src_ref=place,
            dst_ref=place,
            send_sem=recv_sem.at[src_outer, src_inner, part],
            recv_sem=recv_sem.at[src_outer, src_inner, part],
            device_id={"inner": lax.rem(inner + 1, n_inner)},
            device_id_type=MESH,
        ).wait_recv()

    for part in range(CHUNKS):
        pass_on(kv_ref, outer, part, lambda copy: copy.start())

    loads[2].wait()
    pltpu.make_async_copy(q_tiled, q_tiled, load_sem.at[3]).wait()

    here = (outer * n_inner + inner) * 2
    lane = lax.broadcasted_iota(jnp.int32, (tile, tokens), 1)
    tiles = [(group, block) for group in range(groups) for block in range(2)]

    def at(group, block):
        return pl.ds((group * 2 + block) * tile, tile)

    column = lax.broadcasted_iota(jnp.int32, (tile, width), 1)
    for group, block in tiles:
        q_ref[at(group, block), :width] = q_rows[at(group, block), :]
        q_ref[at(group, block), width:] = jnp.where(column == block, 1.0, 0.0).astype(q_ref.dtype)

    def biases(base):
        column = lax.broadcasted_iota(jnp.int32, (span, width), 1)
        halves = []
        for half in range(2):
            bias = [
                jnp.where(span_ref[base + half] < span_ref[here + block], 0.0, MASKED)
                for block in range(2)
            ]
            halves.append(jnp.where(column == 0, bias[0], jnp.where(column == 1, bias[1], 0.0)))
        return jnp.concatenate(halves, axis=0).astype(kv_ref.dtype)

    def scores_of(group, block, place, bias=None):
        keys = place[pl.ds(group * tokens, tokens), :width]
        queries = q_ref[at(group, block), :width]
        if bias is not None:
            keys = jnp.concatenate([keys, bias], axis=1)
            queries = q_ref[at(group, block), :]
        return lax.dot_general(
            queries, keys, (((1,), (1,)), ((), ())), preferred_element_type=jnp.float32
        )

    def attend(group, weights, place):
        return jnp.dot(
            weights.astype(jnp.bfloat16),
            place[pl.ds(group * tokens, tokens), width:],
            preferred_element_type=jnp.float32,
        )

    def visit_own():
        row = lax.broadcasted_iota(jnp.int32, (tile, tokens), 0)
        anchor = jnp.where(lane < span, span_ref[here], span_ref[here + 1])
        ahead = anchor * span + lax.rem(lane, span) - row // group_heads
        scores = scores_of(*tiles[0], kv_ref)
        for index, (group, block) in enumerate(tiles):
            following = None
            if index + 1 < len(tiles):
                following = scores_of(*tiles[index + 1], kv_ref)
            some = at(group, block)
            scores = jnp.where(ahead <= span_ref[here + block] * span, scores, MASKED)
            top = jnp.max(scores, axis=1, keepdims=True)
            weights = jnp.exp2((scores - top) * factor)
            top_ref[some, :] = jnp.broadcast_to(top, (tile, width))
            sum_ref[some, :] = weights[:, :width] + weights[:, width:]
            acc_ref[some, :] = attend(group, weights, kv_ref)
            scores = following

    visit_own()

    def visit(src_outer, src_inner, visited, final=False):
        bias = biases((src_outer * n_inner + src_inner) * 2)
        place = held.at[src_outer, src_inner]

        def settle_sum(some, rescale, added, sums):
            acc = acc_ref[some, :] * rescale + added
            if final:
                total = jnp.sum(sums, axis=1, keepdims=True)
                out_ref[some, :] = (acc / total).astype(o_ref.dtype)
            else:
                acc_ref[some, :] = acc

        scores = scores_of(*visited[0], place, bias)
        waiting = None
        for index, (group, block) in enumerate(visited):
            following = None
            if index + 1 < len(visited):
                following = scores_of(*visited[index + 1], place, bias)
            some = at(group, block)
            left, right = scores[:, :span], scores[:, span:]
            old = top_ref[some, :]
            top = jnp.maximum(old, jnp.max(jnp.maximum(left, right), axis=1, keepdims=True))
            rescale = jnp.exp2((old - top) * factor)
            left = jnp.exp2((left - top) * factor)
            right = jnp.exp2((right - top) * factor)
            sums = sum_ref[some, :] * rescale + (left + right)
            if not final:
                top_ref[some, :] = top
                sum_ref[some, :] = sums
            added = attend(group, jnp.concatenate([left, right], axis=1), place)
            if waiting is not None:
                settle_sum(*waiting)
            waiting = (some, rescale, added, sums)
            scores = following
        settle_sum(*waiting)

    end_outer = jnp.where(outer < n_outer // 2, last, 0)
    first_half, second_half = range(CHUNKS // 2), range(CHUNKS // 2, CHUNKS)
    parts_of = [first_half, second_half]
    tiles_of = [[(group, block) for block in range(2)] for group in range(groups)]

    def take(step, parts):
        for part in parts:
            for side in (1, -1):
                src_outer = outer + side * step

                @pl.when(jnp.logical_and(src_outer >= 0, src_outer < n_outer))
                def _():
                    arrived(src_outer, inner, part)
                    pass_on(
                        held.at[src_outer, inner], src_outer, part, lambda copy: copy.start()
                    )

    def take_far(step):
        for side, end in ((1, last), (-1, 0)):

            @pl.when(outer + side * step == end + side)
            def _():
                for part in second_half:
                    arrived(end, n_inner - 1 - inner, part)
                    far_on(end, part, lambda copy: copy.start())

    def sides(distance, act):
        def one(side, carry):
            src_outer = outer + (1 - 2 * side) * distance

            @pl.when(
                jnp.logical_and(
                    jnp.logical_and(src_outer >= 0, src_outer < n_outer),
                    jnp.logical_and(distance >= 0, jnp.logical_or(distance > 0, side == 0)),
                )
            )
            def _():
                act(src_outer)

            return carry

        lax.fori_loop(0, 2, one, 0)

    def visit_others(src_outer):
        def of_inner(step, carry):
            src_inner = lax.rem(inner + step, n_inner)
            for group in range(groups):
                for part in parts_of[group]:
                    if far_halves and group > 0:

                        @pl.when(jnp.logical_not(is_far(src_outer)))
                        def _():
                            arrived(src_outer, src_inner, part)
                    else:
                        arrived(src_outer, src_inner, part)
                visit(src_outer, src_inner, tiles_of[group])
            return carry

        until = jnp.where(src_outer == end_outer, n_inner - 1, n_inner)
        lax.fori_loop(1, until, of_inner, 0)

    def line_step(step, carry):
        take(step, first_half)
        if far_halves:
            take_far(step)
        sides(step, lambda src_outer: visit(src_outer, inner, tiles_of[0]))
        sides(step - 2 + jnp.where(is_far(outer), 1, 0), visit_others)
        take(step, second_half)
        sides(step, lambda src_outer: visit(src_outer, inner, tiles_of[1]))
        return carry

    lax.fori_loop(1, n_outer, line_step, 0)
    if n_inner > 2:
        sides(jnp.abs(end_outer - outer), visit_others)

    def settle(src_outer, carry):
        for part in range(CHUNKS):
            pass_on(kv_ref, src_outer, part, lambda copy: copy.wait_send())
        return carry

    lax.fori_loop(0, n_outer, settle, 0)
    if far_halves:
        for part in second_half:
            for end in (0, last):
                far_on(end, part, lambda copy: copy.wait_send())

    end_inner = lax.rem(inner + n_inner - 1, n_inner)
    for part in range(CHUNKS):
        if far_halves and part >= CHUNKS // 2:

            @pl.when(is_far(outer))
            def _():
                arrived(end_outer, end_inner, part)
        else:
            arrived(end_outer, end_inner, part)
    visit(end_outer, end_inner, tiles, final=True)


def spread(o_ref, out_hbm, sem):
    copies = [
        pltpu.make_async_copy(o_ref.at[group], out_hbm.at[:, group], sem.at[group])
        for group in range(o_ref.shape[0])
    ]
    for copy in copies:
        copy.start()
    for copy in copies:
        copy.wait()


def solution(mesh):
    n_outer, n_inner = mesh.shape["outer"], mesh.shape["inner"]

    def body(query, key, value, span_order):
        tokens, groups, width = key.shape
        heads = query.shape[1]
        group_heads = heads // groups
        rows = tokens * heads
        by_group = (groups, tokens, group_heads, width)
        kv_shape = (groups * tokens, 2 * width)
        vmem = pl.BlockSpec(memory_space=pltpu.VMEM)
        hbm = pl.BlockSpec(memory_space=pltpu.HBM)
        out = pl.pallas_call(
            functools.partial(kernel, n_outer, n_inner, heads),
            out_shape=jax.ShapeDtypeStruct(by_group, jnp.bfloat16),
            in_specs=[hbm] * 4,
            out_specs=vmem,
            scratch_shapes=[
                pltpu.SMEM(span_order.shape, jnp.int32),
                pltpu.VMEM((groups * tokens, width), jnp.bfloat16),
                pltpu.VMEM((groups * tokens, width), jnp.bfloat16),
                pltpu.VMEM(by_group, jnp.bfloat16),
                pltpu.VMEM((rows, 2 * width), jnp.bfloat16),
                pltpu.VMEM(kv_shape, jnp.bfloat16),
                pltpu.VMEM((n_outer, n_inner) + kv_shape, jnp.bfloat16),
                pltpu.VMEM((rows, width), jnp.float32),
                pltpu.VMEM((rows, width), jnp.float32),
                pltpu.VMEM((rows, width), jnp.float32),
                pltpu.SemaphoreType.DMA((4,)),
                pltpu.SemaphoreType.DMA,
                pltpu.SemaphoreType.DMA((n_outer, n_inner, CHUNKS)),
            ],
            compiler_params=pltpu.CompilerParams(
                collective_id=0, has_side_effects=True, vmem_limit_bytes=VMEM_LIMIT
            ),
        )(
            pltpu.with_memory_space_constraint(span_order, pltpu.HBM),
            pltpu.with_memory_space_constraint(query.reshape(tokens, groups, group_heads, width), pltpu.HBM),
            pltpu.with_memory_space_constraint(key.reshape(groups * tokens, width), pltpu.HBM),
            pltpu.with_memory_space_constraint(value.reshape(groups * tokens, width), pltpu.HBM),
        )
        out = pl.pallas_call(
            spread,
            out_shape=jax.ShapeDtypeStruct((tokens, groups, group_heads, width), jnp.bfloat16),
            in_specs=[vmem],
            out_specs=hbm,
            scratch_shapes=[pltpu.SemaphoreType.DMA((groups,))],
            compiler_params=pltpu.CompilerParams(vmem_limit_bytes=1024 * 1024),
        )(out)
        return out.reshape(query.shape)

    placed = P(("outer", "inner"), "head", None)
    return jax.shard_map(
        body,
        mesh=mesh,
        in_specs=(placed, placed, placed, P()),
        out_specs=placed,
        check_vma=False,
    )
```

```python
import functools
import math

import jax
import jax.numpy as jnp
from jax import lax
from jax.experimental import pallas as pl
from jax.experimental.pallas import tpu as pltpu
from jax.sharding import PartitionSpec as P

MESH = pl.DeviceIdType.MESH
MASKED = -1e30
VMEM_LIMIT = 48 * 1024 * 1024
CHUNKS = 4


def kernel(
    n_outer,
    n_inner,
    heads,
    span_hbm,
    q_hbm,
    key_hbm,
    value_hbm,
    o_ref,
    span_ref,
    key_ref,
    value_ref,
    q_tiled,
    q_ref,
    kv_ref,
    held,
    top_ref,
    sum_ref,
    acc_ref,
    load_sem,
    send_sem,
    recv_sem,
):
    tokens, groups, group_heads, width = q_hbm.shape
    q_rows = q_tiled.reshape(groups * tokens * group_heads, width)
    out_ref = o_ref.reshape(groups * tokens * group_heads, width)
    rows = tokens * group_heads
    span = tokens // 2
    chunk = kv_ref.shape[0] // CHUNKS
    tile = rows // 2
    factor = math.log2(math.e) / math.sqrt(width)
    outer = lax.axis_index("outer")
    inner = lax.axis_index("inner")
    far_halves = n_inner == 2 and n_outer > 2
    last = n_outer - 1

    loads = [
        pltpu.make_async_copy(key_hbm, key_ref, load_sem.at[0]),
        pltpu.make_async_copy(value_hbm, value_ref, load_sem.at[1]),
        pltpu.make_async_copy(span_hbm, span_ref, load_sem.at[2]),
    ]
    for group in range(groups):
        loads.append(
            pltpu.make_async_copy(q_hbm.at[:, group], q_tiled.at[group], load_sem.at[3])
        )
    for load in loads:
        load.start()

    barrier = pltpu.get_barrier_semaphore()

    @pl.when(outer > 0)
    def _():
        pl.semaphore_signal(barrier, inc=1, device_id={"outer": outer - 1}, device_id_type=MESH)

    @pl.when(outer < n_outer - 1)
    def _():
        pl.semaphore_signal(barrier, inc=1, device_id={"outer": outer + 1}, device_id_type=MESH)

    for step in range(1, n_inner):
        peer = lax.rem(inner + step, n_inner)
        pl.semaphore_signal(barrier, inc=1, device_id={"inner": peer}, device_id_type=MESH)

    loads[0].wait()
    loads[1].wait()
    for group in range(groups):
        every = pl.ds(group, tokens, stride=groups)
        here_rows = pl.ds(group * tokens, tokens)
        kv_ref[here_rows, :width] = key_ref[every, :]
        kv_ref[here_rows, width:] = value_ref[every, :]

    ends = jnp.minimum(outer, 1) + jnp.minimum(n_outer - 1 - outer, 1)
    pl.semaphore_wait(barrier, n_inner - 1 + ends)

    def copy_of(source, src_outer, src_inner, part, target):
        return pltpu.make_async_remote_copy(
            src_ref=source.at[pl.ds(part * chunk, chunk)],
            dst_ref=held.at[src_outer, src_inner, pl.ds(part * chunk, chunk)],
            send_sem=send_sem,
            recv_sem=recv_sem.at[src_outer, src_inner, part],
            device_id=target,
            device_id_type=MESH,
        )

    def up(source, src_outer, part):
        return copy_of(source, src_outer, inner, part, {"outer": outer + 1})

    def down(source, src_outer, part):
        return copy_of(source, src_outer, inner, part, {"outer": outer - 1})

    def across(source, src_outer, part, step):
        peer = lax.rem(inner + step, n_inner)
        return copy_of(source, src_outer, inner, part, {"inner": peer})

    def is_far(src_outer):
        return jnp.logical_or(src_outer == 0, src_outer == last)

    def crosses(src_outer, part):
        if not far_halves or part < CHUNKS // 2:
            return jnp.bool_(True)
        return jnp.logical_or(src_outer == outer, jnp.logical_not(is_far(src_outer)))

    def pass_on(source, src_outer, part, act):
        going_up = jnp.logical_and(src_outer <= outer, outer < last)
        going_down = jnp.logical_and(src_outer >= outer, outer > 0)
        upper = outer >= n_outer // 2

        @pl.when(jnp.logical_and(going_up, upper))
        def _():
            act(up(source, src_outer, part))

        @pl.when(going_down)
        def _():
            act(down(source, src_outer, part))

        @pl.when(crosses(src_outer, part))
        def _():
            for step in range(1, n_inner):
                act(across(source, src_outer, part, step))

        @pl.when(jnp.logical_and(going_up, jnp.logical_not(upper)))
        def _():
            act(up(source, src_outer, part))

    def far_on(src_outer, part, act):
        other = n_inner - 1 - inner
        source = held.at[src_outer, other]

        @pl.when(jnp.logical_and(src_outer == 0, outer < last))
        def _():
            act(copy_of(source, 0, other, part, {"outer": outer + 1}))

        @pl.when(jnp.logical_and(src_outer == last, outer > 0))
        def _():
            act(copy_of(source, last, other, part, {"outer": outer - 1}))

    def arrived(src_outer, src_inner, part):
        place = held.at[src_outer, src_inner, pl.ds(part * chunk, chunk)]
        pltpu.make_async_remote_copy(
            src_ref=place,
            dst_ref=place,
            send_sem=recv_sem.at[src_outer, src_inner, part],
            recv_sem=recv_sem.at[src_outer, src_inner, part],
            device_id={"inner": lax.rem(inner + 1, n_inner)},
            device_id_type=MESH,
        ).wait_recv()

    for part in range(CHUNKS):
        pass_on(kv_ref, outer, part, lambda copy: copy.start())

    loads[2].wait()
    pltpu.make_async_copy(q_tiled, q_tiled, load_sem.at[3]).wait()

    here = (outer * n_inner + inner) * 2
    lane = lax.broadcasted_iota(jnp.int32, (tile, tokens), 1)
    tiles = [(group, block) for group in range(groups) for block in range(2)]

    def at(group, block):
        return pl.ds((group * 2 + block) * tile, tile)

    column = lax.broadcasted_iota(jnp.int32, (tile, width), 1)
    for group, block in tiles:
        q_ref[at(group, block), :width] = q_rows[at(group, block), :]
        q_ref[at(group, block), width:] = jnp.where(column == block, 1.0, 0.0).astype(q_ref.dtype)

    def biases(base):
        column = lax.broadcasted_iota(jnp.int32, (span, width), 1)
        halves = []
        for half in range(2):
            bias = [
                jnp.where(span_ref[base + half] < span_ref[here + block], 0.0, MASKED)
                for block in range(2)
            ]
            halves.append(jnp.where(column == 0, bias[0], jnp.where(column == 1, bias[1], 0.0)))
        return jnp.concatenate(halves, axis=0).astype(kv_ref.dtype)

    def scores_of(group, block, place, bias=None):
        keys = place[pl.ds(group * tokens, tokens), :width]
        queries = q_ref[at(group, block), :width]
        if bias is not None:
            keys = jnp.concatenate([keys, bias], axis=1)
            queries = q_ref[at(group, block), :]
        return lax.dot_general(
            queries, keys, (((1,), (1,)), ((), ())), preferred_element_type=jnp.float32
        )

    def attend(group, weights, place):
        return jnp.dot(
            weights.astype(jnp.bfloat16),
            place[pl.ds(group * tokens, tokens), width:],
            preferred_element_type=jnp.float32,
        )

    def visit_own():
        row = lax.broadcasted_iota(jnp.int32, (tile, tokens), 0)
        anchor = jnp.where(lane < span, span_ref[here], span_ref[here + 1])
        ahead = anchor * span + lax.rem(lane, span) - row // group_heads
        scores = scores_of(*tiles[0], kv_ref)
        for index, (group, block) in enumerate(tiles):
            following = None
            if index + 1 < len(tiles):
                following = scores_of(*tiles[index + 1], kv_ref)
            some = at(group, block)
            scores = jnp.where(ahead <= span_ref[here + block] * span, scores, MASKED)
            top = jnp.max(scores, axis=1, keepdims=True)
            weights = jnp.exp2((scores - top) * factor)
            top_ref[some, :] = jnp.broadcast_to(top, (tile, width))
            sum_ref[some, :] = weights[:, :width] + weights[:, width:]
            acc_ref[some, :] = attend(group, weights, kv_ref)
            scores = following

    visit_own()

    def visit(src_outer, src_inner, visited, final=False):
        bias = biases((src_outer * n_inner + src_inner) * 2)
        place = held.at[src_outer, src_inner]

        def settle_sum(some, rescale, added, sums):
            acc = acc_ref[some, :] * rescale + added
            if final:
                total = jnp.sum(sums, axis=1, keepdims=True)
                out_ref[some, :] = (acc / total).astype(o_ref.dtype)
            else:
                acc_ref[some, :] = acc

        scores = scores_of(*visited[0], place, bias)
        waiting = None
        for index, (group, block) in enumerate(visited):
            following = None
            if index + 1 < len(visited):
                following = scores_of(*visited[index + 1], place, bias)
            some = at(group, block)
            left, right = scores[:, :span], scores[:, span:]
            old = top_ref[some, :]
            top = jnp.maximum(old, jnp.max(jnp.maximum(left, right), axis=1, keepdims=True))
            rescale = jnp.exp2((old - top) * factor)
            left = jnp.exp2((left - top) * factor)
            right = jnp.exp2((right - top) * factor)
            sums = sum_ref[some, :] * rescale + (left + right)
            if not final:
                top_ref[some, :] = top
                sum_ref[some, :] = sums
            added = attend(group, jnp.concatenate([left, right], axis=1), place)
            if waiting is not None:
                settle_sum(*waiting)
            waiting = (some, rescale, added, sums)
            scores = following
        settle_sum(*waiting)

    end_outer = jnp.where(outer < n_outer // 2, last, 0)
    first_half, second_half = range(CHUNKS // 2), range(CHUNKS // 2, CHUNKS)
    parts_of = [first_half, second_half]
    tiles_of = [[(group, block) for block in range(2)] for group in range(groups)]

    def take(step, parts):
        for part in parts:
            for side in (1, -1):
                src_outer = outer + side * step

                @pl.when(jnp.logical_and(src_outer >= 0, src_outer < n_outer))
                def _():
                    arrived(src_outer, inner, part)
                    pass_on(
                        held.at[src_outer, inner], src_outer, part, lambda copy: copy.start()
                    )

    def take_far(step):
        for side, end in ((1, last), (-1, 0)):

            @pl.when(outer + side * step == end + side)
            def _():
                for part in second_half:
                    arrived(end, n_inner - 1 - inner, part)
                    far_on(end, part, lambda copy: copy.start())

    def sides(distance, act):
        def one(side, carry):
            src_outer = outer + (1 - 2 * side) * distance

            @pl.when(
                jnp.logical_and(
                    jnp.logical_and(src_outer >= 0, src_outer < n_outer),
                    jnp.logical_and(distance >= 0, jnp.logical_or(distance > 0, side == 0)),
                )
            )
            def _():
                act(src_outer)

            return carry

        lax.fori_loop(0, 2, one, 0)

    def visit_others(src_outer):
        def of_inner(step, carry):
            src_inner = lax.rem(inner + step, n_inner)
            for group in range(groups):
                for part in parts_of[group]:
                    if far_halves and group > 0:

                        @pl.when(jnp.logical_not(is_far(src_outer)))
                        def _():
                            arrived(src_outer, src_inner, part)
                    else:
                        arrived(src_outer, src_inner, part)
                visit(src_outer, src_inner, tiles_of[group])
            return carry

        until = jnp.where(src_outer == end_outer, n_inner - 1, n_inner)
        lax.fori_loop(1, until, of_inner, 0)

    def line_step(step, carry):
        take(step, first_half)
        if far_halves:
            take_far(step)
        sides(step, lambda src_outer: visit(src_outer, inner, tiles_of[0]))
        sides(step - 2 + jnp.where(is_far(outer), 1, 0), visit_others)
        take(step, second_half)
        sides(step, lambda src_outer: visit(src_outer, inner, tiles_of[1]))
        return carry

    lax.fori_loop(1, n_outer, line_step, 0)
    if n_inner > 2 or n_outer % 2 == 1:
        end_distance = jnp.abs(end_outer - outer)

        @pl.when(end_distance >= n_outer - 2)
        def _():
            sides(end_distance, visit_others)

    def settle(src_outer, carry):
        for part in range(CHUNKS):
            pass_on(kv_ref, src_outer, part, lambda copy: copy.wait_send())
        return carry

    lax.fori_loop(0, n_outer, settle, 0)
    if far_halves:
        for part in second_half:
            for end in (0, last):
                far_on(end, part, lambda copy: copy.wait_send())

    end_inner = lax.rem(inner + n_inner - 1, n_inner)
    for part in range(CHUNKS):
        if far_halves and part >= CHUNKS // 2:

            @pl.when(is_far(outer))
            def _():
                arrived(end_outer, end_inner, part)
        else:
            arrived(end_outer, end_inner, part)
    visit(end_outer, end_inner, tiles, final=True)


def spread(o_ref, out_hbm, sem):
    copies = [
        pltpu.make_async_copy(o_ref.at[group], out_hbm.at[:, group], sem.at[group])
        for group in range(o_ref.shape[0])
    ]
    for copy in copies:
        copy.start()
    for copy in copies:
        copy.wait()


def solution(mesh):
    n_outer, n_inner = mesh.shape["outer"], mesh.shape["inner"]

    def body(query, key, value, span_order):
        tokens, groups, width = key.shape
        heads = query.shape[1]
        group_heads = heads // groups
        rows = tokens * heads
        by_group = (groups, tokens, group_heads, width)
        kv_shape = (groups * tokens, 2 * width)
        vmem = pl.BlockSpec(memory_space=pltpu.VMEM)
        hbm = pl.BlockSpec(memory_space=pltpu.HBM)
        out = pl.pallas_call(
            functools.partial(kernel, n_outer, n_inner, heads),
            out_shape=jax.ShapeDtypeStruct(by_group, jnp.bfloat16),
            in_specs=[hbm] * 4,
            out_specs=vmem,
            scratch_shapes=[
                pltpu.SMEM(span_order.shape, jnp.int32),
                pltpu.VMEM((groups * tokens, width), jnp.bfloat16),
                pltpu.VMEM((groups * tokens, width), jnp.bfloat16),
                pltpu.VMEM(by_group, jnp.bfloat16),
                pltpu.VMEM((rows, 2 * width), jnp.bfloat16),
                pltpu.VMEM(kv_shape, jnp.bfloat16),
                pltpu.VMEM((n_outer, n_inner) + kv_shape, jnp.bfloat16),
                pltpu.VMEM((rows, width), jnp.float32),
                pltpu.VMEM((rows, width), jnp.float32),
                pltpu.VMEM((rows, width), jnp.float32),
                pltpu.SemaphoreType.DMA((4,)),
                pltpu.SemaphoreType.DMA,
                pltpu.SemaphoreType.DMA((n_outer, n_inner, CHUNKS)),
            ],
            compiler_params=pltpu.CompilerParams(
                collective_id=0, has_side_effects=True, vmem_limit_bytes=VMEM_LIMIT
            ),
        )(
            pltpu.with_memory_space_constraint(span_order, pltpu.HBM),
            pltpu.with_memory_space_constraint(query.reshape(tokens, groups, group_heads, width), pltpu.HBM),
            pltpu.with_memory_space_constraint(key.reshape(groups * tokens, width), pltpu.HBM),
            pltpu.with_memory_space_constraint(value.reshape(groups * tokens, width), pltpu.HBM),
        )
        out = pl.pallas_call(
            spread,
            out_shape=jax.ShapeDtypeStruct((tokens, groups, group_heads, width), jnp.bfloat16),
            in_specs=[vmem],
            out_specs=hbm,
            scratch_shapes=[pltpu.SemaphoreType.DMA((groups,))],
            compiler_params=pltpu.CompilerParams(vmem_limit_bytes=1024 * 1024),
        )(out)
        return out.reshape(query.shape)

    placed = P(("outer", "inner"), "head", None)
    return jax.shard_map(
        body,
        mesh=mesh,
        in_specs=(placed, placed, placed, P()),
        out_specs=placed,
        check_vma=False,
    )
```

```python
import functools
import math

import jax
import jax.numpy as jnp
from jax import lax
from jax.experimental import pallas as pl
from jax.experimental.pallas import tpu as pltpu
from jax.sharding import PartitionSpec as P

MESH = pl.DeviceIdType.MESH
MASKED = -1e30
VMEM_LIMIT = 48 * 1024 * 1024
CHUNKS = 4


def kernel(
    n_outer,
    n_inner,
    heads,
    span_hbm,
    q_hbm,
    key_hbm,
    value_hbm,
    o_ref,
    span_ref,
    key_ref,
    value_ref,
    q_tiled,
    q_ref,
    kv_ref,
    held,
    top_ref,
    sum_ref,
    acc_ref,
    load_sem,
    send_sem,
    recv_sem,
):
    tokens, groups, group_heads, width = q_hbm.shape
    q_rows = q_tiled.reshape(groups * tokens * group_heads, width)
    out_ref = o_ref.reshape(groups * tokens * group_heads, width)
    rows = tokens * group_heads
    span = tokens // 2
    chunk = kv_ref.shape[0] // CHUNKS
    tile = rows // 2
    factor = math.log2(math.e) / math.sqrt(width)
    outer = lax.axis_index("outer")
    inner = lax.axis_index("inner")
    far_halves = n_inner == 2 and n_outer > 2
    far_parts = range(CHUNKS // 2, CHUNKS)
    last = n_outer - 1

    loads = [
        pltpu.make_async_copy(key_hbm, key_ref, load_sem.at[0]),
        pltpu.make_async_copy(value_hbm, value_ref, load_sem.at[1]),
        pltpu.make_async_copy(span_hbm, span_ref, load_sem.at[2]),
    ]
    for group in range(groups):
        loads.append(
            pltpu.make_async_copy(q_hbm.at[:, group], q_tiled.at[group], load_sem.at[3])
        )
    for load in loads:
        load.start()

    barrier = pltpu.get_barrier_semaphore()

    @pl.when(outer > 0)
    def _():
        pl.semaphore_signal(barrier, inc=1, device_id={"outer": outer - 1}, device_id_type=MESH)

    @pl.when(outer < n_outer - 1)
    def _():
        pl.semaphore_signal(barrier, inc=1, device_id={"outer": outer + 1}, device_id_type=MESH)

    for step in range(1, n_inner):
        peer = lax.rem(inner + step, n_inner)
        pl.semaphore_signal(barrier, inc=1, device_id={"inner": peer}, device_id_type=MESH)

    loads[0].wait()
    loads[1].wait()
    for group in range(groups):
        every = pl.ds(group, tokens, stride=groups)
        here_rows = pl.ds(group * tokens, tokens)
        kv_ref[here_rows, :width] = key_ref[every, :]
        kv_ref[here_rows, width:] = value_ref[every, :]

    ends = jnp.minimum(outer, 1) + jnp.minimum(n_outer - 1 - outer, 1)
    pl.semaphore_wait(barrier, n_inner - 1 + ends)

    def copy_of(source, src_outer, src_inner, part, target):
        return pltpu.make_async_remote_copy(
            src_ref=source.at[pl.ds(part * chunk, chunk)],
            dst_ref=held.at[src_outer, src_inner, pl.ds(part * chunk, chunk)],
            send_sem=send_sem,
            recv_sem=recv_sem.at[src_outer, src_inner, part],
            device_id=target,
            device_id_type=MESH,
        )

    def up(source, src_outer, part):
        return copy_of(source, src_outer, inner, part, {"outer": outer + 1})

    def down(source, src_outer, part):
        return copy_of(source, src_outer, inner, part, {"outer": outer - 1})

    def across(source, src_outer, part, step):
        peer = lax.rem(inner + step, n_inner)
        return copy_of(source, src_outer, inner, part, {"inner": peer})

    def is_far(src_outer):
        return jnp.logical_or(src_outer == 0, src_outer == last)

    def crosses(src_outer, part):
        if not far_halves or part not in far_parts:
            return jnp.bool_(True)
        return jnp.logical_or(src_outer == outer, jnp.logical_not(is_far(src_outer)))

    def pass_on(source, src_outer, part, act):
        going_up = jnp.logical_and(src_outer <= outer, outer < last)
        going_down = jnp.logical_and(src_outer >= outer, outer > 0)
        upper = outer >= n_outer // 2

        @pl.when(jnp.logical_and(going_up, upper))
        def _():
            act(up(source, src_outer, part))

        @pl.when(going_down)
        def _():
            act(down(source, src_outer, part))

        @pl.when(crosses(src_outer, part))
        def _():
            for step in range(1, n_inner):
                act(across(source, src_outer, part, step))

        @pl.when(jnp.logical_and(going_up, jnp.logical_not(upper)))
        def _():
            act(up(source, src_outer, part))

    def far_on(src_outer, part, act):
        other = n_inner - 1 - inner
        source = held.at[src_outer, other]

        @pl.when(jnp.logical_and(src_outer == 0, outer < last))
        def _():
            act(copy_of(source, 0, other, part, {"outer": outer + 1}))

        @pl.when(jnp.logical_and(src_outer == last, outer > 0))
        def _():
            act(copy_of(source, last, other, part, {"outer": outer - 1}))

    def arrived(src_outer, src_inner, part):
        place = held.at[src_outer, src_inner, pl.ds(part * chunk, chunk)]
        pltpu.make_async_remote_copy(
            src_ref=place,
            dst_ref=place,
            send_sem=recv_sem.at[src_outer, src_inner, part],
            recv_sem=recv_sem.at[src_outer, src_inner, part],
            device_id={"inner": lax.rem(inner + 1, n_inner)},
            device_id_type=MESH,
        ).wait_recv()

    for part in range(CHUNKS):
        pass_on(kv_ref, outer, part, lambda copy: copy.start())

    loads[2].wait()
    pltpu.make_async_copy(q_tiled, q_tiled, load_sem.at[3]).wait()

    here = (outer * n_inner + inner) * 2
    lane = lax.broadcasted_iota(jnp.int32, (tile, tokens), 1)
    tiles = [(group, block) for group in range(groups) for block in range(2)]

    def at(group, block):
        return pl.ds((group * 2 + block) * tile, tile)

    column = lax.broadcasted_iota(jnp.int32, (tile, width), 1)
    for group, block in tiles:
        q_ref[at(group, block), :width] = q_rows[at(group, block), :]
        q_ref[at(group, block), width:] = jnp.where(column == block, 1.0, 0.0).astype(q_ref.dtype)

    def biases(base):
        column = lax.broadcasted_iota(jnp.int32, (span, width), 1)
        halves = []
        for half in range(2):
            bias = [
                jnp.where(span_ref[base + half] < span_ref[here + block], 0.0, MASKED)
                for block in range(2)
            ]
            halves.append(jnp.where(column == 0, bias[0], jnp.where(column == 1, bias[1], 0.0)))
        return jnp.concatenate(halves, axis=0).astype(kv_ref.dtype)

    def scores_of(group, block, place, bias=None):
        keys = place[pl.ds(group * tokens, tokens), :width]
        queries = q_ref[at(group, block), :width]
        if bias is not None:
            keys = jnp.concatenate([keys, bias], axis=1)
            queries = q_ref[at(group, block), :]
        return lax.dot_general(
            queries, keys, (((1,), (1,)), ((), ())), preferred_element_type=jnp.float32
        )

    def attend(group, weights, place):
        return jnp.dot(
            weights.astype(jnp.bfloat16),
            place[pl.ds(group * tokens, tokens), width:],
            preferred_element_type=jnp.float32,
        )

    def visit_own():
        row = lax.broadcasted_iota(jnp.int32, (tile, tokens), 0)
        anchor = jnp.where(lane < span, span_ref[here], span_ref[here + 1])
        ahead = anchor * span + lax.rem(lane, span) - row // group_heads
        scores = scores_of(*tiles[0], kv_ref)
        for index, (group, block) in enumerate(tiles):
            following = None
            if index + 1 < len(tiles):
                following = scores_of(*tiles[index + 1], kv_ref)
            some = at(group, block)
            scores = jnp.where(ahead <= span_ref[here + block] * span, scores, MASKED)
            top = jnp.max(scores, axis=1, keepdims=True)
            weights = jnp.exp2((scores - top) * factor)
            top_ref[some, :] = jnp.broadcast_to(top, (tile, width))
            sum_ref[some, :] = weights[:, :width] + weights[:, width:]
            acc_ref[some, :] = attend(group, weights, kv_ref)
            scores = following

    visit_own()

    def visit(blocks, visited, final=False):
        bias = [biases((src_outer * n_inner + src_inner) * 2) for src_outer, src_inner in blocks]
        places = [held.at[src_outer, src_inner] for src_outer, src_inner in blocks]

        def all_scores(index):
            scores = [scores_of(*visited[index], *place) for place in zip(places, bias)]
            return [half for score in scores for half in (score[:, :span], score[:, span:])]

        def settle_sum(some, rescale, added, sums):
            acc = acc_ref[some, :] * rescale + added
            if final:
                total = jnp.sum(sums, axis=1, keepdims=True)
                out_ref[some, :] = (acc / total).astype(o_ref.dtype)
            else:
                acc_ref[some, :] = acc

        scores = all_scores(0)
        waiting = None
        for index, (group, block) in enumerate(visited):
            following = all_scores(index + 1) if index + 1 < len(visited) else None
            some = at(group, block)
            old = top_ref[some, :]
            top = functools.reduce(jnp.maximum, scores)
            top = jnp.maximum(old, jnp.max(top, axis=1, keepdims=True))
            rescale = jnp.exp2((old - top) * factor)
            weights = [jnp.exp2((score - top) * factor) for score in scores]
            sums = sum_ref[some, :] * rescale + sum(weights[1:], weights[0])
            if not final:
                top_ref[some, :] = top
                sum_ref[some, :] = sums
            added = [
                attend(group, jnp.concatenate(weights[2 * k : 2 * k + 2], axis=1), place)
                for k, place in enumerate(places)
            ]
            added = sum(added[1:], added[0])
            if waiting is not None:
                settle_sum(*waiting)
            waiting = (some, rescale, added, sums)
            scores = following
        settle_sum(*waiting)

    end_outer = jnp.where(outer < n_outer // 2, last, 0)
    first_half, second_half = range(CHUNKS // 2), range(CHUNKS // 2, CHUNKS)
    parts_of = [first_half, second_half]
    tiles_of = [[(group, block) for block in range(2)] for group in range(groups)]

    def take(step, parts):
        for part in parts:
            for side in (1, -1):
                src_outer = outer + side * step

                @pl.when(jnp.logical_and(src_outer >= 0, src_outer < n_outer))
                def _():
                    arrived(src_outer, inner, part)
                    pass_on(
                        held.at[src_outer, inner], src_outer, part, lambda copy: copy.start()
                    )

    def take_far(step):
        for side, end in ((1, last), (-1, 0)):

            @pl.when(outer + side * step == end + side)
            def _():
                for part in far_parts:
                    arrived(end, n_inner - 1 - inner, part)
                    far_on(end, part, lambda copy: copy.start())

    def sides(distance, act):
        def one(side, carry):
            src_outer = outer + (1 - 2 * side) * distance

            @pl.when(
                jnp.logical_and(
                    jnp.logical_and(src_outer >= 0, src_outer < n_outer),
                    jnp.logical_and(distance >= 0, jnp.logical_or(distance > 0, side == 0)),
                )
            )
            def _():
                act(src_outer)

            return carry

        lax.fori_loop(0, 2, one, 0)

    def visit_others(src_outer):
        def of_inner(step, carry):
            src_inner = lax.rem(inner + step, n_inner)
            for group in range(groups):
                for part in parts_of[group]:
                    if far_halves and part in far_parts:

                        @pl.when(jnp.logical_not(is_far(src_outer)))
                        def _():
                            arrived(src_outer, src_inner, part)
                    else:
                        arrived(src_outer, src_inner, part)
                visit([(src_outer, src_inner)], tiles_of[group])
            return carry

        until = jnp.where(src_outer == end_outer, n_inner - 1, n_inner)
        lax.fori_loop(1, until, of_inner, 0)

    def pair_at_end(step, group):
        away = jnp.where(outer == 0, 1, -1)
        above, before = outer + away * step, outer + away * (step - 1)
        for part in parts_of[group]:
            if part in far_parts:

                @pl.when(jnp.logical_not(is_far(before)))
                def _():
                    arrived(before, n_inner - 1 - inner, part)
            else:
                arrived(before, n_inner - 1 - inner, part)
        visit([(above, inner), (before, n_inner - 1 - inner)], tiles_of[group])

    def sides_at(step, group):
        sides(step, lambda src_outer: visit([(src_outer, inner)], tiles_of[group]))

    def line_step(step, carry):
        take(step, first_half)
        if far_halves:
            take_far(step)
            pl.when(is_far(outer))(lambda: pair_at_end(step, 0))

            @pl.when(jnp.logical_not(is_far(outer)))
            def _():
                sides_at(step, 0)
                sides(step - 2, visit_others)
        else:
            sides_at(step, 0)
            sides(step - 2 + jnp.where(is_far(outer), 1, 0), visit_others)
        take(step, second_half)
        if far_halves:
            pl.when(is_far(outer))(lambda: pair_at_end(step, 1))
            pl.when(jnp.logical_not(is_far(outer)))(lambda: sides_at(step, 1))
        else:
            sides_at(step, 1)
        return carry

    lax.fori_loop(1, n_outer, line_step, 0)
    if n_inner > 2 or n_outer % 2 == 1:
        end_distance = jnp.abs(end_outer - outer)

        @pl.when(end_distance >= n_outer - 2)
        def _():
            sides(end_distance, visit_others)

    def settle(src_outer, carry):
        for part in range(CHUNKS):
            pass_on(kv_ref, src_outer, part, lambda copy: copy.wait_send())
        return carry

    lax.fori_loop(0, n_outer, settle, 0)
    if far_halves:
        for part in far_parts:
            for end in (0, last):
                far_on(end, part, lambda copy: copy.wait_send())

    end_inner = lax.rem(inner + n_inner - 1, n_inner)
    for part in range(CHUNKS):
        if far_halves and part in far_parts:

            @pl.when(is_far(outer))
            def _():
                arrived(end_outer, end_inner, part)
        else:
            arrived(end_outer, end_inner, part)
    visit([(end_outer, end_inner)], tiles, final=True)


def spread(o_ref, out_hbm, sem):
    copies = [
        pltpu.make_async_copy(o_ref.at[group], out_hbm.at[:, group], sem.at[group])
        for group in range(o_ref.shape[0])
    ]
    for copy in copies:
        copy.start()
    for copy in copies:
        copy.wait()


def solution(mesh):
    n_outer, n_inner = mesh.shape["outer"], mesh.shape["inner"]

    def body(query, key, value, span_order):
        tokens, groups, width = key.shape
        heads = query.shape[1]
        group_heads = heads // groups
        rows = tokens * heads
        by_group = (groups, tokens, group_heads, width)
        kv_shape = (groups * tokens, 2 * width)
        vmem = pl.BlockSpec(memory_space=pltpu.VMEM)
        hbm = pl.BlockSpec(memory_space=pltpu.HBM)
        out = pl.pallas_call(
            functools.partial(kernel, n_outer, n_inner, heads),
            out_shape=jax.ShapeDtypeStruct(by_group, jnp.bfloat16),
            in_specs=[hbm] * 4,
            out_specs=vmem,
            scratch_shapes=[
                pltpu.SMEM(span_order.shape, jnp.int32),
                pltpu.VMEM((groups * tokens, width), jnp.bfloat16),
                pltpu.VMEM((groups * tokens, width), jnp.bfloat16),
                pltpu.VMEM(by_group, jnp.bfloat16),
                pltpu.VMEM((rows, 2 * width), jnp.bfloat16),
                pltpu.VMEM(kv_shape, jnp.bfloat16),
                pltpu.VMEM((n_outer, n_inner) + kv_shape, jnp.bfloat16),
                pltpu.VMEM((rows, width), jnp.float32),
                pltpu.VMEM((rows, width), jnp.float32),
                pltpu.VMEM((rows, width), jnp.float32),
                pltpu.SemaphoreType.DMA((4,)),
                pltpu.SemaphoreType.DMA,
                pltpu.SemaphoreType.DMA((n_outer, n_inner, CHUNKS)),
            ],
            compiler_params=pltpu.CompilerParams(
                collective_id=0, has_side_effects=True, vmem_limit_bytes=VMEM_LIMIT
            ),
        )(
            pltpu.with_memory_space_constraint(span_order, pltpu.HBM),
            pltpu.with_memory_space_constraint(query.reshape(tokens, groups, group_heads, width), pltpu.HBM),
            pltpu.with_memory_space_constraint(key.reshape(groups * tokens, width), pltpu.HBM),
            pltpu.with_memory_space_constraint(value.reshape(groups * tokens, width), pltpu.HBM),
        )
        out = pl.pallas_call(
            spread,
            out_shape=jax.ShapeDtypeStruct((tokens, groups, group_heads, width), jnp.bfloat16),
            in_specs=[vmem],
            out_specs=hbm,
            scratch_shapes=[pltpu.SemaphoreType.DMA((groups,))],
            compiler_params=pltpu.CompilerParams(vmem_limit_bytes=1024 * 1024),
        )(out)
        return out.reshape(query.shape)

    placed = P(("outer", "inner"), "head", None)
    return jax.shard_map(
        body,
        mesh=mesh,
        in_specs=(placed, placed, placed, P()),
        out_specs=placed,
        check_vma=False,
    )
```

```python
import functools
import math

import jax
import jax.numpy as jnp
from jax import lax
from jax.experimental import pallas as pl
from jax.experimental.pallas import tpu as pltpu
from jax.sharding import PartitionSpec as P

MESH = pl.DeviceIdType.MESH
MASKED = -1e30
VMEM_LIMIT = 48 * 1024 * 1024
CHUNKS = 4
PIECES = 8


def kernel(
    n_outer,
    n_inner,
    heads,
    span_hbm,
    q_hbm,
    key_hbm,
    value_hbm,
    o_ref,
    span_ref,
    key_ref,
    value_ref,
    q_tiled,
    q_ref,
    kv_ref,
    held,
    top_ref,
    sum_ref,
    acc_ref,
    load_sem,
    send_sem,
    recv_sem,
):
    tokens, groups, group_heads, width = q_hbm.shape
    q_rows = q_tiled.reshape(groups * tokens * group_heads, width)
    out_ref = o_ref.reshape(groups * tokens * group_heads, width)
    rows = tokens * group_heads
    span = tokens // 2
    chunk = kv_ref.shape[0] // CHUNKS
    tile = rows // 2
    factor = math.log2(math.e) / math.sqrt(width)
    outer = lax.axis_index("outer")
    inner = lax.axis_index("inner")
    far_halves = n_inner == 2 and n_outer > 2
    far_parts = range(CHUNKS // 2, CHUNKS)
    last = n_outer - 1

    loads = [
        pltpu.make_async_copy(key_hbm, key_ref, load_sem.at[0]),
        pltpu.make_async_copy(value_hbm, value_ref, load_sem.at[1]),
        pltpu.make_async_copy(span_hbm, span_ref, load_sem.at[2]),
    ]
    for group in range(groups):
        loads.append(
            pltpu.make_async_copy(q_hbm.at[:, group], q_tiled.at[group], load_sem.at[3])
        )
    for load in loads:
        load.start()

    barrier = pltpu.get_barrier_semaphore()

    @pl.when(outer > 0)
    def _():
        pl.semaphore_signal(barrier, inc=1, device_id={"outer": outer - 1}, device_id_type=MESH)

    @pl.when(outer < n_outer - 1)
    def _():
        pl.semaphore_signal(barrier, inc=1, device_id={"outer": outer + 1}, device_id_type=MESH)

    for step in range(1, n_inner):
        peer = lax.rem(inner + step, n_inner)
        pl.semaphore_signal(barrier, inc=1, device_id={"inner": peer}, device_id_type=MESH)

    loads[0].wait()
    loads[1].wait()
    for group in range(groups):
        every = pl.ds(group, tokens, stride=groups)
        here_rows = pl.ds(group * tokens, tokens)
        kv_ref[here_rows, :width] = key_ref[every, :]
        kv_ref[here_rows, width:] = value_ref[every, :]

    ends = jnp.minimum(outer, 1) + jnp.minimum(n_outer - 1 - outer, 1)
    pl.semaphore_wait(barrier, n_inner - 1 + ends)

    def copy_of(source, src_outer, src_inner, part, target):
        return pltpu.make_async_remote_copy(
            src_ref=source.at[pl.ds(part * chunk, chunk)],
            dst_ref=held.at[src_outer, src_inner, pl.ds(part * chunk, chunk)],
            send_sem=send_sem,
            recv_sem=recv_sem.at[src_outer, src_inner, part],
            device_id=target,
            device_id_type=MESH,
        )

    def up(source, src_outer, part):
        return copy_of(source, src_outer, inner, part, {"outer": outer + 1})

    def down(source, src_outer, part):
        return copy_of(source, src_outer, inner, part, {"outer": outer - 1})

    def across(source, src_outer, part, step):
        peer = lax.rem(inner + step, n_inner)
        return copy_of(source, src_outer, inner, part, {"inner": peer})

    def is_far(src_outer):
        return jnp.logical_or(src_outer == 0, src_outer == last)

    def crosses(src_outer, part):
        if not far_halves or part not in far_parts:
            return jnp.bool_(True)
        return jnp.logical_or(src_outer == outer, jnp.logical_not(is_far(src_outer)))

    def pass_on(source, src_outer, part, act):
        going_up = jnp.logical_and(src_outer <= outer, outer < last)
        going_down = jnp.logical_and(src_outer >= outer, outer > 0)
        upper = outer >= n_outer // 2

        @pl.when(jnp.logical_and(going_up, upper))
        def _():
            act(up(source, src_outer, part))

        @pl.when(going_down)
        def _():
            act(down(source, src_outer, part))

        @pl.when(crosses(src_outer, part))
        def _():
            for step in range(1, n_inner):
                act(across(source, src_outer, part, step))

        @pl.when(jnp.logical_and(going_up, jnp.logical_not(upper)))
        def _():
            act(up(source, src_outer, part))

    def far_on(src_outer, part, act):
        other = n_inner - 1 - inner
        source = held.at[src_outer, other]

        @pl.when(jnp.logical_and(src_outer == 0, outer < last))
        def _():
            act(copy_of(source, 0, other, part, {"outer": outer + 1}))

        @pl.when(jnp.logical_and(src_outer == last, outer > 0))
        def _():
            act(copy_of(source, last, other, part, {"outer": outer - 1}))

    def arrived(src_outer, src_inner, part):
        place = held.at[src_outer, src_inner, pl.ds(part * chunk, chunk)]
        pltpu.make_async_remote_copy(
            src_ref=place,
            dst_ref=place,
            send_sem=recv_sem.at[src_outer, src_inner, part],
            recv_sem=recv_sem.at[src_outer, src_inner, part],
            device_id={"inner": lax.rem(inner + 1, n_inner)},
            device_id_type=MESH,
        ).wait_recv()

    for part in range(CHUNKS):
        pass_on(kv_ref, outer, part, lambda copy: copy.start())

    loads[2].wait()
    pltpu.make_async_copy(q_tiled, q_tiled, load_sem.at[3]).wait()

    here = (outer * n_inner + inner) * 2
    lane = lax.broadcasted_iota(jnp.int32, (tile, tokens), 1)
    tiles = [(group, block) for group in range(groups) for block in range(2)]

    def at(group, block):
        return pl.ds((group * 2 + block) * tile, tile)

    column = lax.broadcasted_iota(jnp.int32, (tile, width), 1)
    for group, block in tiles:
        q_ref[at(group, block), :width] = q_rows[at(group, block), :]
        q_ref[at(group, block), width:] = jnp.where(column == block, 1.0, 0.0).astype(q_ref.dtype)

    def biases(base):
        column = lax.broadcasted_iota(jnp.int32, (span, width), 1)
        halves = []
        for half in range(2):
            bias = [
                jnp.where(span_ref[base + half] < span_ref[here + block], 0.0, MASKED)
                for block in range(2)
            ]
            halves.append(jnp.where(column == 0, bias[0], jnp.where(column == 1, bias[1], 0.0)))
        return jnp.concatenate(halves, axis=0).astype(kv_ref.dtype)

    def scores_of(group, block, place, bias=None):
        keys = place[pl.ds(group * tokens, tokens), :width]
        queries = q_ref[at(group, block), :width]
        if bias is not None:
            keys = jnp.concatenate([keys, bias], axis=1)
            queries = q_ref[at(group, block), :]
        return lax.dot_general(
            queries, keys, (((1,), (1,)), ((), ())), preferred_element_type=jnp.float32
        )

    def attend(group, weights, place):
        return jnp.dot(
            weights.astype(jnp.bfloat16),
            place[pl.ds(group * tokens, tokens), width:],
            preferred_element_type=jnp.float32,
        )

    def visit_own():
        row = lax.broadcasted_iota(jnp.int32, (tile, tokens), 0)
        anchor = jnp.where(lane < span, span_ref[here], span_ref[here + 1])
        ahead = anchor * span + lax.rem(lane, span) - row // group_heads
        scores = scores_of(*tiles[0], kv_ref)
        for index, (group, block) in enumerate(tiles):
            following = None
            if index + 1 < len(tiles):
                following = scores_of(*tiles[index + 1], kv_ref)
            some = at(group, block)
            scores = jnp.where(ahead <= span_ref[here + block] * span, scores, MASKED)
            top = jnp.max(scores, axis=1, keepdims=True)
            weights = jnp.exp2((scores - top) * factor)
            top_ref[some, :] = jnp.broadcast_to(top, (tile, width))
            sum_ref[some, :] = weights[:, :width] + weights[:, width:]
            acc_ref[some, :] = attend(group, weights, kv_ref)
            scores = following

    visit_own()

    def visit(blocks, visited, final=False):
        bias = [biases((src_outer * n_inner + src_inner) * 2) for src_outer, src_inner in blocks]
        places = [held.at[src_outer, src_inner] for src_outer, src_inner in blocks]

        def all_scores(index):
            scores = [scores_of(*visited[index], *place) for place in zip(places, bias)]
            return [half for score in scores for half in (score[:, :span], score[:, span:])]

        def settle_sum(some, rescale, added, sums):
            acc = acc_ref[some, :] * rescale + added
            if final:
                total = jnp.sum(sums, axis=1, keepdims=True)
                out_ref[some, :] = (acc / total).astype(o_ref.dtype)
            else:
                acc_ref[some, :] = acc

        scores = all_scores(0)
        waiting = None
        for index, (group, block) in enumerate(visited):
            following = all_scores(index + 1) if index + 1 < len(visited) else None
            some = at(group, block)
            old = top_ref[some, :]
            top = functools.reduce(jnp.maximum, scores)
            top = jnp.maximum(old, jnp.max(top, axis=1, keepdims=True))
            rescale = jnp.exp2((old - top) * factor)
            weights = [jnp.exp2((score - top) * factor) for score in scores]
            sums = sum_ref[some, :] * rescale + sum(weights[1:], weights[0])
            if not final:
                top_ref[some, :] = top
                sum_ref[some, :] = sums
            added = [
                attend(group, jnp.concatenate(weights[2 * k : 2 * k + 2], axis=1), place)
                for k, place in enumerate(places)
            ]
            added = sum(added[1:], added[0])
            if waiting is not None:
                settle_sum(*waiting)
            waiting = (some, rescale, added, sums)
            scores = following
        settle_sum(*waiting)

    end_outer = jnp.where(outer < n_outer // 2, last, 0)
    first_half, second_half = range(CHUNKS // 2), range(CHUNKS // 2, CHUNKS)
    parts_of = [first_half, second_half]
    tiles_of = [[(group, block) for block in range(2)] for group in range(groups)]

    def take(step, parts):
        for part in parts:
            for side in (1, -1):
                src_outer = outer + side * step

                @pl.when(jnp.logical_and(src_outer >= 0, src_outer < n_outer))
                def _():
                    arrived(src_outer, inner, part)
                    pass_on(
                        held.at[src_outer, inner], src_outer, part, lambda copy: copy.start()
                    )

    def take_far(step):
        for side, end in ((1, last), (-1, 0)):

            @pl.when(outer + side * step == end + side)
            def _():
                for part in far_parts:
                    arrived(end, n_inner - 1 - inner, part)
                    far_on(end, part, lambda copy: copy.start())

    def sides(distance, act):
        def one(side, carry):
            src_outer = outer + (1 - 2 * side) * distance

            @pl.when(
                jnp.logical_and(
                    jnp.logical_and(src_outer >= 0, src_outer < n_outer),
                    jnp.logical_and(distance >= 0, jnp.logical_or(distance > 0, side == 0)),
                )
            )
            def _():
                act(src_outer)

            return carry

        lax.fori_loop(0, 2, one, 0)

    def visit_others(src_outer):
        def of_inner(step, carry):
            src_inner = lax.rem(inner + step, n_inner)
            for group in range(groups):
                for part in parts_of[group]:
                    if far_halves and part in far_parts:

                        @pl.when(jnp.logical_not(is_far(src_outer)))
                        def _():
                            arrived(src_outer, src_inner, part)
                    else:
                        arrived(src_outer, src_inner, part)
                visit([(src_outer, src_inner)], tiles_of[group])
            return carry

        until = jnp.where(src_outer == end_outer, n_inner - 1, n_inner)
        lax.fori_loop(1, until, of_inner, 0)

    def pair_at_end(step, group):
        away = jnp.where(outer == 0, 1, -1)
        above, before = outer + away * step, outer + away * (step - 1)
        for part in parts_of[group]:
            if part in far_parts:

                @pl.when(jnp.logical_not(is_far(before)))
                def _():
                    arrived(before, n_inner - 1 - inner, part)
            else:
                arrived(before, n_inner - 1 - inner, part)
        visit([(above, inner), (before, n_inner - 1 - inner)], tiles_of[group])

    def sides_at(step, group):
        sides(step, lambda src_outer: visit([(src_outer, inner)], tiles_of[group]))

    def line_step(step, carry):
        take(step, first_half)
        if far_halves:
            take_far(step)
            pl.when(is_far(outer))(lambda: pair_at_end(step, 0))

            @pl.when(jnp.logical_not(is_far(outer)))
            def _():
                sides_at(step, 0)
                sides(step - 2, visit_others)
        else:
            sides_at(step, 0)
            sides(step - 2 + jnp.where(is_far(outer), 1, 0), visit_others)
        take(step, second_half)
        if far_halves:
            pl.when(is_far(outer))(lambda: pair_at_end(step, 1))
            pl.when(jnp.logical_not(is_far(outer)))(lambda: sides_at(step, 1))
        else:
            sides_at(step, 1)
        return carry

    lax.fori_loop(1, n_outer, line_step, 0)
    if n_inner > 2 or n_outer % 2 == 1:
        end_distance = jnp.abs(end_outer - outer)

        @pl.when(end_distance >= n_outer - 2)
        def _():
            sides(end_distance, visit_others)

    def settle(src_outer, carry):
        for part in range(CHUNKS):
            pass_on(kv_ref, src_outer, part, lambda copy: copy.wait_send())
        return carry

    lax.fori_loop(0, n_outer, settle, 0)
    if far_halves:
        for part in far_parts:
            for end in (0, last):
                far_on(end, part, lambda copy: copy.wait_send())

    end_inner = lax.rem(inner + n_inner - 1, n_inner)
    for part in range(CHUNKS):
        if far_halves and part in far_parts:

            @pl.when(is_far(outer))
            def _():
                arrived(end_outer, end_inner, part)
        else:
            arrived(end_outer, end_inner, part)
    visit([(end_outer, end_inner)], tiles, final=True)


def spread(o_ref, out_hbm, sem):
    groups, tokens = o_ref.shape[:2]
    some = tokens // PIECES
    for first in range(0, tokens, some):
        for group in range(groups):
            pltpu.make_async_copy(
                o_ref.at[group, pl.ds(first, some)], out_hbm.at[pl.ds(first, some), group], sem
            ).start()
    pltpu.make_async_copy(o_ref, o_ref, sem).wait()


def solution(mesh):
    n_outer, n_inner = mesh.shape["outer"], mesh.shape["inner"]

    def body(query, key, value, span_order):
        tokens, groups, width = key.shape
        heads = query.shape[1]
        group_heads = heads // groups
        rows = tokens * heads
        by_group = (groups, tokens, group_heads, width)
        kv_shape = (groups * tokens, 2 * width)
        vmem = pl.BlockSpec(memory_space=pltpu.VMEM)
        hbm = pl.BlockSpec(memory_space=pltpu.HBM)
        out = pl.pallas_call(
            functools.partial(kernel, n_outer, n_inner, heads),
            out_shape=jax.ShapeDtypeStruct(by_group, jnp.bfloat16),
            in_specs=[hbm] * 4,
            out_specs=vmem,
            scratch_shapes=[
                pltpu.SMEM(span_order.shape, jnp.int32),
                pltpu.VMEM((groups * tokens, width), jnp.bfloat16),
                pltpu.VMEM((groups * tokens, width), jnp.bfloat16),
                pltpu.VMEM(by_group, jnp.bfloat16),
                pltpu.VMEM((rows, 2 * width), jnp.bfloat16),
                pltpu.VMEM(kv_shape, jnp.bfloat16),
                pltpu.VMEM((n_outer, n_inner) + kv_shape, jnp.bfloat16),
                pltpu.VMEM((rows, width), jnp.float32),
                pltpu.VMEM((rows, width), jnp.float32),
                pltpu.VMEM((rows, width), jnp.float32),
                pltpu.SemaphoreType.DMA((4,)),
                pltpu.SemaphoreType.DMA,
                pltpu.SemaphoreType.DMA((n_outer, n_inner, CHUNKS)),
            ],
            compiler_params=pltpu.CompilerParams(
                collective_id=0, has_side_effects=True, vmem_limit_bytes=VMEM_LIMIT
            ),
        )(
            pltpu.with_memory_space_constraint(span_order, pltpu.HBM),
            pltpu.with_memory_space_constraint(query.reshape(tokens, groups, group_heads, width), pltpu.HBM),
            pltpu.with_memory_space_constraint(key.reshape(groups * tokens, width), pltpu.HBM),
            pltpu.with_memory_space_constraint(value.reshape(groups * tokens, width), pltpu.HBM),
        )
        out = pl.pallas_call(
            spread,
            out_shape=jax.ShapeDtypeStruct((tokens, groups, group_heads, width), jnp.bfloat16),
            in_specs=[vmem],
            out_specs=hbm,
            scratch_shapes=[pltpu.SemaphoreType.DMA],
            compiler_params=pltpu.CompilerParams(vmem_limit_bytes=1024 * 1024),
        )(out)
        return out.reshape(query.shape)

    placed = P(("outer", "inner"), "head", None)
    return jax.shard_map(
        body,
        mesh=mesh,
        in_specs=(placed, placed, placed, P()),
        out_specs=placed,
        check_vma=False,
    )
```
